128 devices in a mesh: gx: 8 (over y, core), gy: 16 (over x, z).
Axes of the slice: x: 4, y: 4, z: 4, core: 2. Of those that a mesh axis runs over, the one named last changes fastest.
Arguments:
- right_side: float32 [512, 512, 512], P('gx', 'gy'), may hold values from -120 to 120
- diagonal: float32 [512, 512, 512], P('gx', 'gy'), may hold values from 0.002 to 0.2
Outputs:
- update: float32 [512, 512, 512], P('gx', 'gy')
- residual: float32 [512, 512, 512], P('gx', 'gy')
The draws below stay inside these ranges and needn't reach their ends.
All inputs are finite; a program needn't handle non-finite values.
Results may differ from the reference program's by a relative error of at most 0.00028.
Values sent between devices are 32-bit elements; how exact they have to be, the bound alone decides.
No kernel may reach another device: no remote copies, remote signals or barrier semaphores. Data moves between devices by JAX's collectives and lax.ppermute only.
A program may use at most 128 MiB of HBM per device.

```python
import math
import jax
import jax.numpy as jnp
from jax import lax

CZ = 512
NX = 512
NY = 512


def draw_right_side(key, part):
    noise = jnp.clip(jax.random.normal(key, (NX, NY, CZ), jnp.float32), -6.0, 6.0)
    along_x = jnp.arange(NX, dtype=jnp.float32) / NX
    along_y = jnp.arange(NY, dtype=jnp.float32) / NY
    scale = (1.0 + 0.75 * along_x)[:, None, None] * (1.0 + 0.75 * along_y)[None, :, None]
    return noise * scale


def level_of(own_key, shape, pieces, smallest, top_value):
    level, own = 1.0, jax.random.fold_in(own_key, 6)
    for position, parts in pieces:
        heights = jnp.exp(jax.random.uniform(jax.random.fold_in(own, position), (parts,), jnp.float32, smallest / len(pieces), top_value / len(pieces)))
        level = level * jnp.repeat(heights, shape[position] // parts).reshape([-1 if axis == position else 1 for axis in range(len(shape))])
    return level


def setup_inputs(seed: int = 0) -> dict:
    key_list = jax.random.split(jax.random.key(seed), 3)
    return {
        "right_side": draw_right_side(jax.random.fold_in(key_list[2], 71), 0),
        "diagonal": jnp.clip(jnp.exp(math.log(0.2) - 4.6051702 * jax.random.uniform(key_list[1], (NX, NY, CZ), jnp.float32) ** level_of(key_list[1], (NX, NY, CZ), ((0, 8), (1, 16)), -0.2, 0.2)), 0.002, 0.2),
    }


relax_weight = 0.8
coarse_sweeps = 8


def neighbour_sum(padded):
    total = padded[2:, 1:-1, 1:-1] + padded[:-2, 1:-1, 1:-1]
    total = total + padded[1:-1, 2:, 1:-1] + padded[1:-1, :-2, 1:-1]
    return total + padded[1:-1, 1:-1, 2:] + padded[1:-1, 1:-1, :-2]


def level_operator(field, padded, coefficient, level):
    return (6.0 * field - neighbour_sum(padded)) * (0.25 ** level) + coefficient * field


def zero_pad(field):
    return jnp.pad(field, 1)


def pair_table(depth):
    fine_index = jnp.arange(depth, dtype=jnp.int32)[:, None] // 2
    coarse_index = jnp.arange(depth // 2, dtype=jnp.int32)[None, :]
    return jnp.where(fine_index == coarse_index, 1.0, 0.0).astype(jnp.float32)


def restrict(field):
    first, second, third = field.shape
    halved = jnp.dot(field.reshape(first * second, third), 0.5 * pair_table(third), precision=lax.Precision.HIGHEST)
    halved = halved.reshape(first // 2, 2, second // 2, 2, third // 2)
    return halved.sum(axis=(1, 3)) * 0.25


def prolong(field):
    first, second, third = field.shape
    doubled = jnp.dot(field.reshape(first * second, third), pair_table(2 * third).T, precision=lax.Precision.HIGHEST)
    doubled = doubled.reshape(first, 1, second, 1, 2 * third)
    doubled = jnp.broadcast_to(doubled, (first, 2, second, 2, 2 * third))
    return doubled.reshape(2 * first, 2 * second, 2 * third)


def smooth(residual, coefficient, level, padder):
    inverse = relax_weight / (6.0 * 0.25 ** level + coefficient)
    guess = inverse * residual
    return guess + inverse * (residual - level_operator(guess, padder(guess), coefficient, level))


def coarse_solve(residual, coefficient):
    inverse = relax_weight / (6.0 * 0.25 ** 3 + coefficient)
    guess = jnp.zeros_like(residual)
    for sweep_index in range(coarse_sweeps):
        guess = guess + inverse * (residual - level_operator(guess, zero_pad(guess), coefficient, 3))
    leftover = residual - level_operator(guess, zero_pad(guess), coefficient, 3)
    ones_field = jnp.ones_like(residual)
    ones_image = level_operator(ones_field, zero_pad(ones_field), coefficient, 3)
    shift = jnp.sum(leftover) / jnp.sum(ones_image)
    return guess + shift


def reference(right_side, diagonal):
    mid_res = restrict(right_side)
    mid_coef = restrict(diagonal)
    low_res = restrict(mid_res)
    low_coef = restrict(mid_coef)
    base_res = restrict(low_res)
    base_coef = restrict(low_coef)
    base_sol = coarse_solve(base_res, base_coef)
    low_sol = smooth(low_res, low_coef, 2, zero_pad) + prolong(base_sol)
    mid_sol = smooth(mid_res, mid_coef, 1, zero_pad) + prolong(low_sol)
    precond = smooth(right_side, diagonal, 0, zero_pad) + prolong(mid_sol)
    image = level_operator(precond, zero_pad(precond), diagonal, 0)
    alpha = jnp.sum(right_side * precond) / jnp.sum(precond * image)
    return alpha * precond, right_side - alpha * image
```

```python
import jax
import jax.numpy as jnp
from jax import lax
from jax.experimental import pallas as pl
from jax.experimental.pallas import tpu as pltpu
from jax.sharding import PartitionSpec as P

F32 = jnp.float32
BF16 = jnp.bfloat16

X, Y, Z = 64, 32, 512
DEVS_X, DEVS_Y = 8, 16
WHOLE = 512
LANES = 128
CHUNK = 8

XF, XM, XL, XB, XROWS = 0, 384, 480, 504, 536
YM, YL, YB, YC, YROWS = 0, 192, 240, 336, 352


def iota(shape, axis):
    return lax.broadcasted_iota(jnp.int32, shape, axis)


def halving(depth, cols, offset=0):
    coarse = lax.shift_right_logical(iota((depth, cols), 0), 1) + offset
    return jnp.where(coarse == iota((depth, cols), 1), 0.125, 0.0).astype(BF16)


def doubling(depth, cols):
    coarse = lax.shift_right_logical(iota((depth, cols), 1), 1)
    return jnp.where(coarse == iota((depth, cols), 0), 1.0, 0.0).astype(BF16)


def times(value, table):
    high = value.astype(BF16)
    low = (value - high.astype(F32)).astype(BF16)
    return jnp.dot(high, table, preferred_element_type=F32) + jnp.dot(low, table, preferred_element_type=F32)


def in_plane(c, top, bottom):
    rows, lanes = c.shape
    row, lane = iota(c.shape, 0), iota(c.shape, 1)
    up = jnp.where(row == 0, top, pltpu.roll(c, 1, 0))
    down = jnp.where(row == rows - 1, bottom, pltpu.roll(c, rows - 1, 0))
    left = jnp.where(lane == 0, 0.0, pltpu.roll(c, 1, 1))
    right = jnp.where(lane == lanes - 1, 0.0, pltpu.roll(c, lanes - 1, 1))
    return (up + down) + (left + right)


def cols(k):
    return slice(LANES * k, LANES * (k + 1))


def take(ref, rows):
    return jnp.concatenate([ref[k, rows, :] for k in range(ref.shape[0])], axis=1)


def put(ref, rows, value):
    for k in range(ref.shape[0]):
        ref[k, rows, :] = value[:, cols(k)]


def parities():
    gx, gy = lax.axis_index("gx"), lax.axis_index("gy")
    return gx % 2, gy % 2, (gy // 2) % 2


def restrict_kernel(r_hbm, d_hbm, r_v, d_v, s0, sx, syf, sys, s1, s2,
                    g_s, i_s, rm, cm, gm, im, rl, cl, gl, il, sems):
    px, py, _ = parities()

    def copies(c):
        rows = pl.ds(c * CHUNK * Y, CHUNK * Y)
        for n, (src, dst) in enumerate(((r_hbm, r_v), (d_hbm, d_v))):
            for k in range(4):
                yield pltpu.make_async_copy(src.at[rows, pl.ds(LANES * k, LANES)], dst.at[k, rows], sems.at[n, c, k])

    for c in range(X // CHUNK):
        for one in copies(c):
            one.start()

    for k in range(4):
        g_s[k, pl.ds(0, Y), :] = jnp.zeros((Y, LANES), F32)
        g_s[k, pl.ds((X + 1) * Y, Y), :] = jnp.zeros((Y, LANES), F32)
    for k in range(2):
        gm[k, pl.ds(0, 16), :] = jnp.zeros((16, LANES), F32)
        gm[k, pl.ds(33 * 16, 16), :] = jnp.zeros((16, LANES), F32)
    half = halving(512, 256)

    def load(c, carry):
        for one in copies(c):
            one.wait()
        base = c * CHUNK * Y

        def plane(i, carry):
            rows = pl.ds(base + i * Y, Y)
            inv = 0.8 / (6.0 + take(d_v, rows))
            put(i_s, rows, inv)
            put(g_s, pl.ds(base + (i + 1) * Y, Y), inv * take(r_v, rows))
            return carry

        lax.fori_loop(0, CHUNK, plane, 0)
        n = CHUNK * Y // 2
        for src, dst in ((r_v, rm), (d_v, cm)):
            pairs = jnp.concatenate(
                [src[k, pl.ds(base, n, 2), :] + src[k, pl.ds(base + 1, n, 2), :] for k in range(4)], axis=1)
            pairs = pairs.reshape(CHUNK // 2, 2, 16, Z)
            pairs = (pairs[:, 0] + pairs[:, 1]).reshape(CHUNK // 2 * 16, Z)
            put(dst, pl.ds(c * (CHUNK // 2 * 16), CHUNK // 2 * 16), times(pairs, half))
        return carry

    lax.fori_loop(0, X // CHUNK, load, 0)

    half = halving(256, 128)
    for src, dst in ((rm, rl), (cm, cl)):
        pairs = jnp.concatenate([src[k, pl.ds(0, 256, 2), :] + src[k, pl.ds(1, 256, 2), :] for k in range(2)], axis=1)
        pairs = pairs.reshape(16, 2, 8, 256)
        pairs = (pairs[:, 0] + pairs[:, 1]).reshape(128, 256)
        dst[...] = times(pairs, half)
    packed = 0.0
    for src, offset in ((rl, 0), (cl, 64)):
        quad = [sum(src[pl.ds(8 * f + 2 * j + e, 8, 16), :] for e in range(2) for f in range(2)) for j in range(4)]
        packed = packed + times(jnp.concatenate(quad, axis=0), halving(128, 128, offset))
    for slot in range(2):
        sx[slot, pl.ds(XB, 32), :] = packed

    inv = 0.8 / (0.09375 * 4.0 + cl[...])
    il[...] = inv
    gl[...] = inv * rl[...]
    for i in range(16):
        rows = pl.ds(8 * i, 8)
        c = gl[rows, :]
        total = in_plane(c, 0.0, 0.0)
        if i > 0:
            total = total + gl[pl.ds(8 * i - 8, 8), :]
        if i < 15:
            total = total + gl[pl.ds(8 * i + 8, 8), :]
        s2[rows, :] = il[rows, :] * (1.2 * rl[rows, :] + 0.0625 * total)

    def guess(i, carry):
        rows = pl.ds(64 * i, 64)
        inv = 0.8 / (1.5 + take(cm, rows))
        put(im, rows, inv)
        put(gm, pl.ds(64 * i + 16, 64), inv * take(rm, rows))
        return carry

    lax.fori_loop(0, 8, guess, 0)

    def middle(i, carry):
        rows = pl.ds(16 * i, 16)
        c = take(gm, pl.ds(16 * i + 16, 16))
        total = in_plane(c, 0.0, 0.0) + (take(gm, rows) + take(gm, pl.ds(16 * i + 32, 16)))
        put(s1, rows, take(im, rows) * (1.2 * take(rm, rows) + 0.25 * total))
        return carry

    lax.fori_loop(0, 32, middle, 0, unroll=4)

    def fine(i, carry):
        rows = pl.ds(Y * i, Y)
        c = take(g_s, pl.ds(Y * i + Y, Y))
        total = in_plane(c, 0.0, 0.0) + (take(g_s, rows) + take(g_s, pl.ds(Y * i + 2 * Y, Y)))
        put(s0, rows, take(i_s, rows) * (1.2 * take(r_v, rows) + total))
        return carry

    lax.fori_loop(0, X, fine, 0, unroll=2)

    for hi in range(2):
        slot = px if hi else 1 - px
        for a, (ref, pad) in enumerate(((g_s, Y), (i_s, 0), (s0, 0))):
            for k in range(4):
                sx[slot, pl.ds(XF + (4 * a + k) * Y, Y), :] = ref[k, pl.ds(pad + hi * (X - 1) * Y, Y), :]
        for a, (ref, pad) in enumerate(((gm, 16), (im, 0), (s1, 0))):
            for k in range(2):
                sx[slot, pl.ds(XM + (2 * a + k) * 16, 16), :] = ref[k, pl.ds(pad + hi * 31 * 16, 16), :]
        for a, ref in enumerate((gl, il, s2)):
            sx[slot, pl.ds(XL + a * 8, 8), :] = ref[pl.ds(hi * 15 * 8, 8), :]
        slot = py if hi else 1 - py
        for a, (ref, pad) in enumerate(((g_s, Y), (i_s, 0), (s0, 0))):
            for k in range(4):
                syf[slot, pl.ds((4 * a + k) * X, X), :] = ref[k, pl.ds(pad + hi * (Y - 1), X, Y), :]
        for a, (ref, pad) in enumerate(((gm, 16), (im, 0), (s1, 0))):
            for k in range(2):
                sys[slot, pl.ds(YM + (2 * a + k) * 32, 32), :] = ref[k, pl.ds(pad + hi * 15, 32, 16), :]
        for a, ref in enumerate((gl, il, s2)):
            sys[slot, pl.ds(YL + a * 16, 16), :] = ref[pl.ds(hi * 7, 16, 8), :]


def pick(slot, first, second, rows):
    return jnp.where(slot == 0, first[rows, :], second[rows, :])


def pack_kernel(sx, rxa, rxb, sys, block, out):
    px, py, _ = parities()
    for j in range(4):
        rows = pl.ds(XB + 8 * j, 8)
        block[pl.ds(24 * j, 8), :] = pick(1 - px, rxa, rxb, rows)
        block[pl.ds(24 * j + 8, 8), :] = sx[0, rows, :]
        block[pl.ds(24 * j + 16, 8), :] = pick(px, rxa, rxb, rows)
    for hi in range(2):
        slot = py if hi else 1 - py
        out[slot, pl.ds(0, YB), :] = sys[slot, pl.ds(0, YB), :]
        out[slot, pl.ds(YB, 96), :] = block[...]
        corner = []
        for xside in range(2):
            own = px if xside else 1 - px
            for base, n, ks in ((XF, Y, 4), (XM, 16, 2), (XL, 8, 1)):
                for k in range(ks):
                    corner.append(pick(own, rxa, rxb, pl.ds(base + k * n + hi * (n - 1), 1)))
        corner.append(jnp.zeros((2, LANES), F32))
        out[slot, pl.ds(YC, 16), :] = jnp.concatenate(corner, axis=0)


def solve_kernel(r_v, d_v, s0, s1, s2, sx, syf, sys, block, rxa, rxb, rya, ryb, rsa, rsb, r2a, r2b,
                 p, im, sums,
                 bs, ga, gb, sz, low_s, rep_l, mid_s, rep_m, fl, fm, hy):
    px, py, qy = parities()

    ysel = (lambda hi: py if hi else 1 - py)
    q = (lambda hi: qy if hi else 1 - qy)
    low2, low1 = pick(q(0), r2a, r2b, slice(None)), pick(ysel(0), rsa, rsb, pl.ds(YB, 96))
    high1, high2 = pick(ysel(1), rsa, rsb, pl.ds(YB, 96)), pick(q(1), r2a, r2b, slice(None))
    for n, part in enumerate((low2, low1, block[...], high1, high2)):
        bs[pl.ds(4 * n, 4)] = part.reshape(4, 24, LANES)
    shape = (20, 24, LANES)
    live = iota(shape, 2) < 64
    both = bs[...]
    res = jnp.where(live, both, 0.0)
    coef = jnp.where(live, pltpu.roll(both, 64, 2), 0.0)
    inv = jnp.where(coef > 0.0, 0.8 / (0.09375 + coef), 0.0)
    zero = jnp.zeros((24, LANES), F32)
    for ref in (ga, gb):
        ref[0] = zero
        ref[21] = zero

    def around(ref):
        c = ref[pl.ds(1, 20)]
        total = ref[pl.ds(0, 20)] + ref[pl.ds(2, 20)]
        total = total + (pltpu.roll(c, 1, 1) + pltpu.roll(c, 23, 1))
        return c, total + (pltpu.roll(c, 1, 2) + pltpu.roll(c, LANES - 1, 2))

    ga[pl.ds(1, 20)] = inv * res
    bs[...] = inv
    now, new = ga, gb
    for sweep in range(7):
        c, total = around(now)
        new[pl.ds(1, 20)] = c + bs[...] * (res - ((0.09375 + coef) * c - 0.015625 * total))
        now, new = new, now
    c, total = around(now)
    left = res - ((0.09375 + coef) * c - 0.015625 * total)
    leftover = jnp.sum(jnp.where(live[8:12, 8:16], left[8:12, 8:16], 0.0))
    sz[...] = times(now[pl.ds(8, 6)].reshape(144, LANES), doubling(LANES, LANES))

    def hx(hi, start, n):
        return pick(px if hi else 1 - px, rxa, rxb, pl.ds(start, n))

    def hyf(hi, start, n):
        return pick(ysel(hi), rya, ryb, pl.ds(start, n))

    def hys(hi, start, n):
        return pick(ysel(hi), rsa, rsb, pl.ds(start, n))

    def ox(hi, start, n):
        return sx[px if hi else 1 - px, pl.ds(start, n), :]

    def oyf(hi, start, n):
        return syf[ysel(hi), pl.ds(start, n), :]

    def oys(hi, start, n):
        return sys[ysel(hi), pl.ds(start, n), :]

    for j in range(4):
        for e in range(2):
            for f in range(2):
                low_s[pl.ds(8 * f + 2 * j + e, 8, 16), :] = sz[pl.ds(24 * (j + 1) + 8, 8), :]
    low_s[...] = low_s[...] + s2[...]
    for hi in range(2):
        rows = pl.ds(hi * 120, 8)
        low_s[rows, :] = low_s[rows, :] + 0.0625 * ox(hi, XL + 8, 8) * hx(hi, XL, 8)
    for hi in range(2):
        rows = pl.ds(hi * 7, 16, 8)
        low_s[rows, :] = low_s[rows, :] + 0.0625 * oys(hi, YL + 16, 16) * hys(hi, YL, 16)

    rep_l[pl.ds(0, 128, 2), :] = low_s[...]
    rep_l[pl.ds(1, 128, 2), :] = low_s[...]
    wide = times(rep_l[...], doubling(128, 256)).reshape(16, 1, 16, 256)
    wide = jnp.broadcast_to(wide, (16, 2, 16, 256)).reshape(512, 256)
    for k in range(2):
        mid_s[k] = wide[:, cols(k)] + s1[k]
    for hi in range(2):
        for k in range(2):
            rows = pl.ds(hi * 496, 16)
            mid_s[k, rows, :] = mid_s[k, rows, :] + 0.25 * ox(hi, XM + 32 + 16 * k, 16) * hx(hi, XM + 16 * k, 16)
    for hi in range(2):
        for k in range(2):
            rows = pl.ds(hi * 15, 32, 16)
            mid_s[k, rows, :] = mid_s[k, rows, :] + 0.25 * oys(hi, YM + 64 + 32 * k, 32) * hys(hi, YM + 32 * k, 32)

    for k in range(2):
        rep_m[k, pl.ds(0, 512, 2), :] = mid_s[k]
        rep_m[k, pl.ds(1, 512, 2), :] = mid_s[k]
    twice = doubling(256, Z)

    def spread(i, carry):
        wide = times(take(rep_m, pl.ds(128 * i, 128)), twice).reshape(4, 1, Y, Z)
        wide = jnp.broadcast_to(wide, (4, 2, Y, Z)).reshape(8 * Y, Z)
        for k in range(4):
            p[k, pl.ds(8 * Y * i + Y, 8 * Y), :] = wide[:, cols(k)] + s0[k, pl.ds(8 * Y * i, 8 * Y), :]
        return carry

    lax.fori_loop(0, 8, spread, 0)
    for hi in range(2):
        for k in range(4):
            rows = pl.ds(Y + hi * (X - 1) * Y, Y)
            p[k, rows, :] = p[k, rows, :] + ox(hi, XF + (4 + k) * Y, Y) * hx(hi, XF + k * Y, Y)
    for hi in range(2):
        for k in range(4):
            rows = pl.ds(Y + hi * (Y - 1), X, Y)
            p[k, rows, :] = p[k, rows, :] + oyf(hi, (4 + k) * X, X) * hyf(hi, k * X, X)

    def corner(yhi, xhi, level, k):
        return hys(yhi, YC + 7 * xhi + (0, 4, 6)[level] + k, 1)

    def ends(n, first, last):
        row = iota((n, LANES), 0)
        return jnp.where(row == 0, first, jnp.where(row == n - 1, last, 0.0))

    def beyond(along_y, hi):
        n = X if along_y else Y

        def diag(level, k, rows):
            if along_y:
                return ends(rows, corner(hi, 0, level, k), corner(hi, 1, level, k))
            return ends(rows, corner(0, hi, level, k), corner(1, hi, level, k))

        lo, md, fi = (hys, hys, hyf) if along_y else (hx, hx, hx)
        olo, omd, ofi = (oys, oys, oyf) if along_y else (ox, ox, ox)
        bl, bm, bf = (YL, YM, 0) if along_y else (XL, XM, XF)
        n2, n1 = n // 4, n // 2
        if along_y:
            top = sz[pl.ds(120 * hi + 8, 8), :]
        else:
            top = sz[pl.ds(24 + (16 if hi else 7), 4, 24), :]
        fl[pl.ds(0, n2 // 2, 2), :] = top
        fl[pl.ds(1, n2 // 2, 2), :] = top
        near = olo(hi, bl, n2) + diag(2, 0, n2)
        low = lo(hi, bl + 2 * n2, n2) + 0.0625 * lo(hi, bl + n2, n2) * near + fl[pl.ds(0, n2), :]
        fl[pl.ds(0, n2, 2), :] = low
        fl[pl.ds(1, n2, 2), :] = low
        wide = times(fl[pl.ds(0, n1), :], doubling(128, 256))
        for k in range(2):
            near = omd(hi, bm + k * n1, n1) + diag(1, k, n1)
            mid = md(hi, bm + (4 + k) * n1, n1) + 0.25 * md(hi, bm + (2 + k) * n1, n1) * near + wide[:, cols(k)]
            fm[k, pl.ds(0, n1, 2), :] = mid
            fm[k, pl.ds(1, n1, 2), :] = mid
        wide = times(take(fm, pl.ds(0, n)), twice)
        out = []
        for k in range(4):
            near = ofi(hi, bf + k * n, n) + diag(0, k, n)
            inv = fi(hi, bf + (4 + k) * n, n)
            fine = fi(hi, bf + (8 + k) * n, n) + inv * near + wide[:, cols(k)]
            out.append(jnp.where(inv > 0.0, fine, 0.0))
        return jnp.concatenate(out, axis=1)

    put(p, pl.ds(0, Y), beyond(False, 0))
    put(p, pl.ds((X + 1) * Y, Y), beyond(False, 1))
    hy[0] = beyond(True, 0)
    hy[1] = beyond(True, 1)

    def fold(v):
        v = (v[0:8] + v[8:16]) + (v[16:24] + v[24:32])
        return (v[:, cols(0)] + v[:, cols(1)]) + (v[:, cols(2)] + v[:, cols(3)])

    def image(i, carry):
        rows = pl.ds(Y * i, Y)
        c = take(p, pl.ds(Y * i + Y, Y))
        around = in_plane(c, hy[0, pl.ds(i, 1), :], hy[1, pl.ds(i, 1), :])
        around = around + (take(p, rows) + take(p, pl.ds(Y * i + 2 * Y, Y)))
        dd, rr = take(d_v, rows), take(r_v, rows)
        out = (6.0 + dd) * c - around
        im[rows, :] = out
        return tuple(t + fold(v) for t, v in zip(carry, (rr * c, c * out, rr, out, dd)))

    start = jnp.zeros((8, LANES), F32)
    totals = lax.fori_loop(0, X, image, (start,) * 5)
    totals = [jnp.sum(t) for t in totals] + [leftover]
    lane = iota((LANES, 8), 1)
    packed = jnp.zeros((LANES, 8), F32)
    for n, t in enumerate(totals):
        packed = jnp.where(lane == n, t, packed)
    sums[...] = packed


def final_kernel(every, r_v, d_v, p, im, update, residual):
    step = pl.program_id(0)
    gx, gy = lax.axis_index("gx"), lax.axis_index("gy")
    total = jnp.sum(every[...], axis=0, keepdims=True)
    lane8 = iota((1, 8), 1)
    rz, zq, res_sum, image_sum, coef_sum, left = [jnp.sum(jnp.where(lane8 == n, total, 0.0), axis=1, keepdims=True) for n in range(6)]
    shift = left / (coef_sum / 512.0 + 6.0 * 64.0 * 64.0 / 64.0)
    ones_sum = coef_sum + 6.0 * WHOLE * WHOLE
    alpha = (rz + shift * res_sum) / (zq + shift * (2.0 * image_sum + shift * ones_sum))
    scaled = alpha * shift
    row, lane = iota((Y, Z), 0), iota((Y, Z), 1)
    walls = jnp.where(lane == 0, 1.0, 0.0) + jnp.where(lane == Z - 1, 1.0, 0.0)
    walls = walls + jnp.where((row == 0) & (gy == 0), 1.0, 0.0)
    walls = walls + jnp.where((row == Y - 1) & (gy == DEVS_Y - 1), 1.0, 0.0)

    def plane(i, carry):
        x = step * CHUNK + i
        end = ((x == 0) & (gx == 0)) | ((x == X - 1) & (gx == DEVS_X - 1))
        rows = pl.ds(x * Y, Y)
        outside = walls + jnp.where(end, 1.0, 0.0)
        here = pl.ds(i * Y, Y)
        update[here, :] = alpha * take(p, pl.ds(x * Y + Y, Y)) + scaled
        residual[here, :] = take(r_v, rows) - alpha * im[rows, :] - scaled * (take(d_v, rows) + outside)
        return carry

    lax.fori_loop(0, CHUNK, plane, 0, unroll=2)


def f32(*shape):
    return jax.ShapeDtypeStruct(shape, F32)


def resident(*shape):
    return pltpu.VMEM(shape, F32)


def in_vmem(value):
    return pltpu.with_memory_space_constraint(value, pltpu.VMEM)


VM = pl.BlockSpec(memory_space=pltpu.VMEM)


def swap(value, axis, distance, offset):
    count = lax.axis_size(axis)
    pairs = []
    for i in range(count - distance):
        if (i // distance) % 2 == offset:
            pairs += [(i, i + distance), (i + distance, i)]
    return lax.ppermute(value, axis, pairs)


def body(right_side, diagonal):
    r = right_side.reshape(X * Y, Z)
    d = diagonal.reshape(X * Y, Z)
    vm = pltpu.VMEM
    r_v, d_v, s0, sx, syf, sys, s1, s2 = pl.pallas_call(
        restrict_kernel,
        in_specs=[pl.BlockSpec(memory_space=pl.ANY)] * 2,
        out_specs=[VM] * 8,
        out_shape=[resident(4, X * Y, LANES)] * 3 + [f32(2, XROWS, LANES), f32(2, 768, LANES), f32(2, YB, LANES), f32(2, 512, LANES), f32(128, 128)],
        scratch_shapes=[vm((4, (X + 2) * Y, LANES), F32), vm((4, X * Y, LANES), F32), vm((2, 512, LANES), F32), vm((2, 512, LANES), F32),
                        vm((2, 544, LANES), F32), vm((2, 512, LANES), F32)] + [vm((128, 128), F32)] * 4
        + [pltpu.SemaphoreType.DMA((2, X // CHUNK, 4))],
        compiler_params=pltpu.CompilerParams(vmem_limit_bytes=40 * 2**20),
        name="restrict_all",
    )(r, d)

    rxa = swap(sx[0], "gx", 1, 0)
    rxb = swap(sx[1], "gx", 1, 1)
    block, small = pl.pallas_call(
        pack_kernel,
        in_specs=[VM] * 4,
        out_specs=[VM] * 2,
        out_shape=[f32(96, LANES), f32(2, YROWS, LANES)],
        name="pack_faces",
    )(sx, rxa, rxb, sys)
    r2a = swap(block, "gy", 2, 0)
    r2b = swap(block, "gy", 2, 1)
    rsa = swap(small[0], "gy", 1, 0)
    rsb = swap(small[1], "gy", 1, 1)
    rya = swap(syf[0], "gy", 1, 0)
    ryb = swap(syf[1], "gy", 1, 1)

    p, im, sums = pl.pallas_call(
        solve_kernel,
        in_specs=[VM] * 17,
        out_specs=[VM] * 3,
        out_shape=[resident(4, (X + 2) * Y, LANES), resident(X * Y, Z), f32(LANES, 8)],
        scratch_shapes=[vm((20, 24, LANES), F32), vm((22, 24, LANES), F32), vm((22, 24, LANES), F32), vm((144, LANES), F32),
                        vm((128, 128), F32), vm((256, 128), F32), vm((2, 512, LANES), F32), vm((2, 1024, LANES), F32),
                        vm((32, LANES), F32), vm((2, X, LANES), F32), vm((2, X, Z), F32)],
        compiler_params=pltpu.CompilerParams(vmem_limit_bytes=40 * 2**20),
        name="solve_levels",
    )(in_vmem(r_v), in_vmem(d_v), in_vmem(s0), s1, s2, sx, syf, sys, block, rxa, rxb, rya, ryb, rsa, rsb, r2a, r2b)

    every = lax.all_to_all(sums, ("gx", "gy"), 0, 0, tiled=True)
    blocks = pl.BlockSpec((CHUNK * Y, Z), lambda i: (i, 0))
    update, residual = pl.pallas_call(
        final_kernel,
        grid=(X // CHUNK,),
        in_specs=[VM] * 5,
        out_specs=[blocks, blocks],
        out_shape=[f32(X * Y, Z), f32(X * Y, Z)],
        compiler_params=pltpu.CompilerParams(vmem_limit_bytes=30 * 2**20),
        name="scale_outputs",
    )(every, in_vmem(r_v), in_vmem(d_v), in_vmem(p), in_vmem(im))
    return update.reshape(X, Y, Z), residual.reshape(X, Y, Z)


def solution(mesh):
    return jax.shard_map(
        body,
        mesh=mesh,
        in_specs=(P("gx", "gy", None), P("gx", "gy", None)),
        out_specs=(P("gx", "gy", None), P("gx", "gy", None)),
        check_vma=False,
    )
```

```python
import jax
import jax.numpy as jnp
from jax import lax
from jax.experimental import pallas as pl
from jax.experimental.pallas import tpu as pltpu
from jax.sharding import PartitionSpec as P

F32 = jnp.float32
BF16 = jnp.bfloat16

X, Y, Z = 64, 32, 512
DEVS_X, DEVS_Y = 8, 16
WHOLE = 512
LANES = 128
COST = 20_000_000
CHUNK = 8

XF, XM, XL, XB, XROWS = 0, 384, 480, 504, 536
YM, YL, YB, YC, YROWS = 0, 192, 240, 336, 352


def iota(shape, axis):
    return lax.broadcasted_iota(jnp.int32, shape, axis)


def halving(depth, cols, offset=0):
    coarse = lax.shift_right_logical(iota((depth, cols), 0), 1) + offset
    return jnp.where(coarse == iota((depth, cols), 1), 0.125, 0.0).astype(BF16)


def doubling(depth, cols):
    coarse = lax.shift_right_logical(iota((depth, cols), 1), 1)
    return jnp.where(coarse == iota((depth, cols), 0), 1.0, 0.0).astype(BF16)


def times(value, table):
    high = value.astype(BF16)
    low = (value - high.astype(F32)).astype(BF16)
    return jnp.dot(high, table, preferred_element_type=F32) + jnp.dot(low, table, preferred_element_type=F32)


def in_plane(c, top, bottom):
    rows, lanes = c.shape
    row, lane = iota(c.shape, 0), iota(c.shape, 1)
    up = jnp.where(row == 0, top, pltpu.roll(c, 1, 0))
    down = jnp.where(row == rows - 1, bottom, pltpu.roll(c, rows - 1, 0))
    left = jnp.where(lane == 0, 0.0, pltpu.roll(c, 1, 1))
    right = jnp.where(lane == lanes - 1, 0.0, pltpu.roll(c, lanes - 1, 1))
    return (up + down) + (left + right)


def cols(k):
    return slice(LANES * k, LANES * (k + 1))


def take(ref, rows):
    return jnp.concatenate([ref[k, rows, :] for k in range(ref.shape[0])], axis=1)


def put(ref, rows, value):
    for k in range(ref.shape[0]):
        ref[k, rows, :] = value[:, cols(k)]


def send(parity, first, second, rows, low, high):
    first[rows, :] = jnp.where(parity == 0, high, low)
    second[rows, :] = jnp.where(parity == 0, low, high)


def parities():
    gx, gy = lax.axis_index("gx"), lax.axis_index("gy")
    return gx % 2, gy % 2, (gy // 2) % 2


def restrict_kernel(r_hbm, d_hbm, r_v, d_v, g_s, i_s, sxa, sxb, sma, smb, s1, s2,
                    rm, cm, gm, im, rl, cl, gl, il, sems):
    px, py, _ = parities()

    def copies(c):
        rows = pl.ds(c * CHUNK * Y, CHUNK * Y)
        for n, (src, dst) in enumerate(((r_hbm, r_v), (d_hbm, d_v))):
            for k in range(4):
                yield pltpu.make_async_copy(src.at[rows, pl.ds(LANES * k, LANES)], dst.at[k, rows], sems.at[n, c, k])

    for c in range(X // CHUNK):
        for one in copies(c):
            one.start()

    for k in range(4):
        g_s[k, pl.ds(0, Y), :] = jnp.zeros((Y, LANES), F32)
        g_s[k, pl.ds((X + 1) * Y, Y), :] = jnp.zeros((Y, LANES), F32)
    for k in range(2):
        gm[k, pl.ds(0, 16), :] = jnp.zeros((16, LANES), F32)
        gm[k, pl.ds(33 * 16, 16), :] = jnp.zeros((16, LANES), F32)
    half = halving(512, 256)

    def load(c, carry):
        for one in copies(c):
            one.wait()
        base = c * CHUNK * Y

        def plane(i, carry):
            rows = pl.ds(base + i * Y, Y)
            inv = 0.8 / (6.0 + take(d_v, rows))
            put(i_s, rows, inv)
            put(g_s, pl.ds(base + (i + 1) * Y, Y), inv * take(r_v, rows))
            return carry

        lax.fori_loop(0, CHUNK, plane, 0)
        n = CHUNK * Y // 2
        for src, dst in ((r_v, rm), (d_v, cm)):
            pairs = jnp.concatenate(
                [src[k, pl.ds(base, n, 2), :] + src[k, pl.ds(base + 1, n, 2), :] for k in range(4)], axis=1)
            pairs = pairs.reshape(CHUNK // 2, 2, 16, Z)
            pairs = (pairs[:, 0] + pairs[:, 1]).reshape(CHUNK // 2 * 16, Z)
            put(dst, pl.ds(c * (CHUNK // 2 * 16), CHUNK // 2 * 16), times(pairs, half))
        return carry

    lax.fori_loop(0, X // CHUNK, load, 0)

    half = halving(256, 128)
    for src, dst in ((rm, rl), (cm, cl)):
        pairs = jnp.concatenate([src[k, pl.ds(0, 256, 2), :] + src[k, pl.ds(1, 256, 2), :] for k in range(2)], axis=1)
        pairs = pairs.reshape(16, 2, 8, 256)
        pairs = (pairs[:, 0] + pairs[:, 1]).reshape(128, 256)
        dst[...] = times(pairs, half)
    packed = 0.0
    for src, offset in ((rl, 0), (cl, 64)):
        quad = [sum(src[pl.ds(8 * f + 2 * j + e, 8, 16), :] for e in range(2) for f in range(2)) for j in range(4)]
        packed = packed + times(jnp.concatenate(quad, axis=0), halving(128, 128, offset))
    sxa[pl.ds(XB, 32), :] = packed
    sxb[pl.ds(XB, 32), :] = packed

    inv = 0.8 / (0.09375 * 4.0 + cl[...])
    il[...] = inv
    gl[...] = inv * rl[...]
    for i in range(16):
        rows = pl.ds(8 * i, 8)
        c = gl[rows, :]
        total = in_plane(c, 0.0, 0.0)
        if i > 0:
            total = total + gl[pl.ds(8 * i - 8, 8), :]
        if i < 15:
            total = total + gl[pl.ds(8 * i + 8, 8), :]
        s2[rows, :] = il[rows, :] * (1.2 * rl[rows, :] + 0.0625 * total)

    def guess(i, carry):
        rows = pl.ds(64 * i, 64)
        inv = 0.8 / (1.5 + take(cm, rows))
        put(im, rows, inv)
        put(gm, pl.ds(64 * i + 16, 64), inv * take(rm, rows))
        return carry

    lax.fori_loop(0, 8, guess, 0)

    def middle(i, carry):
        rows = pl.ds(16 * i, 16)
        c = take(gm, pl.ds(16 * i + 16, 16))
        total = in_plane(c, 0.0, 0.0) + (take(gm, rows) + take(gm, pl.ds(16 * i + 32, 16)))
        put(s1, rows, take(im, rows) * (1.2 * take(rm, rows) + 0.25 * total))
        return carry

    lax.fori_loop(0, 32, middle, 0, unroll=4)

    ends = []
    for i, near in ((0, 1), (X - 1, X - 2)):
        rows = pl.ds(Y * i, Y)
        g, inv = take(g_s, pl.ds(Y * i + Y, Y)), take(i_s, rows)
        total = in_plane(g, 0.0, 0.0) + take(g_s, pl.ds(Y * near + Y, Y))
        ends.append((g, inv, inv * (1.2 * take(r_v, rows) + total)))
    for a in range(3):
        for k in range(4):
            send(px, sxa, sxb, pl.ds(XF + (4 * a + k) * Y, Y), ends[0][a][:, cols(k)], ends[1][a][:, cols(k)])
    for a, (ref, pad) in enumerate(((gm, 16), (im, 0), (s1, 0))):
        for k in range(2):
            send(px, sxa, sxb, pl.ds(XM + (2 * a + k) * 16, 16),
                 ref[k, pl.ds(pad, 16), :], ref[k, pl.ds(pad + 31 * 16, 16), :])
            send(py, sma, smb, pl.ds(YM + (2 * a + k) * 32, 32),
                 ref[k, pl.ds(pad, 32, 16), :], ref[k, pl.ds(pad + 15, 32, 16), :])
    for a, ref in enumerate((gl, il, s2)):
        send(px, sxa, sxb, pl.ds(XL + a * 8, 8), ref[pl.ds(0, 8), :], ref[pl.ds(15 * 8, 8), :])
        send(py, sma, smb, pl.ds(YL + a * 16, 16), ref[pl.ds(0, 16, 8), :], ref[pl.ds(7, 16, 8), :])


def smooth_kernel(r_v, g_s, i_s, s0, sya, syb):
    _, py, _ = parities()

    def fine(i, carry):
        rows = pl.ds(Y * i, Y)
        c = take(g_s, pl.ds(Y * i + Y, Y))
        total = in_plane(c, 0.0, 0.0) + (take(g_s, rows) + take(g_s, pl.ds(Y * i + 2 * Y, Y)))
        put(s0, rows, take(i_s, rows) * (1.2 * take(r_v, rows) + total))
        return carry

    lax.fori_loop(0, X, fine, 0)
    for a, (ref, pad) in enumerate(((g_s, Y), (i_s, 0), (s0, 0))):
        for k in range(4):
            send(py, sya, syb, pl.ds((4 * a + k) * X, X),
                 ref[k, pl.ds(pad, X, Y), :], ref[k, pl.ds(pad + Y - 1, X, Y), :])


def pick(slot, first, second, rows):
    return jnp.where(slot == 0, first[rows, :], second[rows, :])


def pack_kernel(sxa, rxa, rxb, sma, smb, block, outa, outb):
    px, py, _ = parities()
    for j in range(4):
        rows = pl.ds(XB + 8 * j, 8)
        block[pl.ds(24 * j, 8), :] = pick(1 - px, rxa, rxb, rows)
        block[pl.ds(24 * j + 8, 8), :] = sxa[rows, :]
        block[pl.ds(24 * j + 16, 8), :] = pick(px, rxa, rxb, rows)
    for src, out in ((sma, outa), (smb, outb)):
        out[pl.ds(0, YB), :] = src[...]
        out[pl.ds(YB, 96), :] = block[...]
    rows = []
    for hi in range(2):
        corner = []
        for xside in range(2):
            own = px if xside else 1 - px
            for base, n, ks in ((XF, Y, 4), (XM, 16, 2), (XL, 8, 1)):
                for k in range(ks):
                    corner.append(pick(own, rxa, rxb, pl.ds(base + k * n + hi * (n - 1), 1)))
        corner.append(jnp.zeros((2, LANES), F32))
        rows.append(jnp.concatenate(corner, axis=0))
    low, high = rows
    outa[pl.ds(YC, 16), :] = jnp.where(py == 0, high, low)
    outb[pl.ds(YC, 16), :] = jnp.where(py == 0, low, high)


class Halo:
    def __init__(self, sx, sy, sm, rx, ry, rs):
        self.px, self.py, _ = parities()
        self.pairs = dict(sx=sx, sy=sy, sm=sm, rx=rx, ry=ry, rs=rs)

    def get(self, name, hi, start, n):
        parity = self.px if name in ("sx", "rx") else self.py
        return pick(parity if hi else 1 - parity, *self.pairs[name], pl.ds(start, n))

    def diag(self, along_y, hi, level, k, rows):
        ends = []
        for other in range(2):
            yhi, xhi = (hi, other) if along_y else (other, hi)
            ends.append(self.get("rs", yhi, YC + 7 * xhi + (0, 4, 6)[level] + k, 1))
        row = iota((rows, LANES), 0)
        return jnp.where(row == 0, ends[0], jnp.where(row == rows - 1, ends[1], 0.0))


FACES = ((False, 0), (False, 1), (True, 0), (True, 1))
FACE_ROWS = (0, Y, 2 * Y, 2 * Y + X)


def coarse_kernel(s1, s2, sxa, sxb, sma, smb, block, rxa, rxb, rsa, rsb, r2a, r2b,
                  rep_m, fm, left_out,
                  bs, ga, gb, sz, low_s, rep_l, mid_s, fl):
    px, py, qy = parities()
    halo = Halo((sxa, sxb), None, (sma, smb), (rxa, rxb), None, (rsa, rsb))

    ysel = (lambda hi: py if hi else 1 - py)
    q = (lambda hi: qy if hi else 1 - qy)
    low2, low1 = pick(q(0), r2a, r2b, slice(None)), pick(ysel(0), rsa, rsb, pl.ds(YB, 96))
    high1, high2 = pick(ysel(1), rsa, rsb, pl.ds(YB, 96)), pick(q(1), r2a, r2b, slice(None))
    for n, part in enumerate((low2, low1, block[...], high1, high2)):
        bs[pl.ds(4 * n, 4)] = part.reshape(4, 24, LANES)
    shape = (20, 24, LANES)
    live = iota(shape, 2) < 64
    both = bs[...]
    res = jnp.where(live, both, 0.0)
    coef = jnp.where(live, pltpu.roll(both, 64, 2), 0.0)
    inv = jnp.where(coef > 0.0, 0.8 / (0.09375 + coef), 0.0)
    zero = jnp.zeros((24, LANES), F32)
    for ref in (ga, gb):
        ref[0] = zero
        ref[21] = zero

    def around(ref):
        c = ref[pl.ds(1, 20)]
        total = ref[pl.ds(0, 20)] + ref[pl.ds(2, 20)]
        total = total + (pltpu.roll(c, 1, 1) + pltpu.roll(c, 23, 1))
        return c, total + (pltpu.roll(c, 1, 2) + pltpu.roll(c, LANES - 1, 2))

    ga[pl.ds(1, 20)] = inv * res
    bs[...] = inv
    now, new = ga, gb
    for sweep in range(7):
        c, total = around(now)
        new[pl.ds(1, 20)] = c + bs[...] * (res - ((0.09375 + coef) * c - 0.015625 * total))
        now, new = new, now
    c, total = around(now)
    left = res - ((0.09375 + coef) * c - 0.015625 * total)
    leftover = jnp.sum(jnp.where(live[8:12, 8:16], left[8:12, 8:16], 0.0))
    sz[...] = times(now[pl.ds(8, 6)].reshape(144, LANES), doubling(LANES, LANES))

    left_out[...] = jnp.full((8, LANES), leftover, F32)

    for j in range(4):
        for e in range(2):
            for f in range(2):
                low_s[pl.ds(8 * f + 2 * j + e, 8, 16), :] = sz[pl.ds(24 * (j + 1) + 8, 8), :]
    low_s[...] = low_s[...] + s2[...]
    for hi in range(2):
        rows = pl.ds(hi * 120, 8)
        low_s[rows, :] = low_s[rows, :] + 0.0625 * halo.get("sx", hi, XL + 8, 8) * halo.get("rx", hi, XL, 8)
    for hi in range(2):
        rows = pl.ds(hi * 7, 16, 8)
        low_s[rows, :] = low_s[rows, :] + 0.0625 * halo.get("sm", hi, YL + 16, 16) * halo.get("rs", hi, YL, 16)

    rep_l[pl.ds(0, 128, 2), :] = low_s[...]
    rep_l[pl.ds(1, 128, 2), :] = low_s[...]
    wide = times(rep_l[...], doubling(128, 256)).reshape(16, 1, 16, 256)
    wide = jnp.broadcast_to(wide, (16, 2, 16, 256)).reshape(512, 256)
    for k in range(2):
        mid_s[k] = wide[:, cols(k)] + s1[k]
    for hi in range(2):
        for k in range(2):
            rows = pl.ds(hi * 496, 16)
            mid_s[k, rows, :] = mid_s[k, rows, :] + (
                0.25 * halo.get("sx", hi, XM + 32 + 16 * k, 16) * halo.get("rx", hi, XM + 16 * k, 16))
    for hi in range(2):
        for k in range(2):
            rows = pl.ds(hi * 15, 32, 16)
            mid_s[k, rows, :] = mid_s[k, rows, :] + (
                0.25 * halo.get("sm", hi, YM + 64 + 32 * k, 32) * halo.get("rs", hi, YM + 32 * k, 32))

    for k in range(2):
        rep_m[k, pl.ds(0, 512, 2), :] = mid_s[k]
        rep_m[k, pl.ds(1, 512, 2), :] = mid_s[k]
    for (along_y, hi), base in zip(FACES, FACE_ROWS):
        n = X if along_y else Y
        theirs, own, bl, bm = ("rs", "sm", YL, YM) if along_y else ("rx", "sx", XL, XM)
        n2, n1 = n // 4, n // 2
        if along_y:
            top = sz[pl.ds(120 * hi + 8, 8), :]
        else:
            top = sz[pl.ds(24 + (16 if hi else 7), 4, 24), :]
        fl[pl.ds(0, n2 // 2, 2), :] = top
        fl[pl.ds(1, n2 // 2, 2), :] = top
        near = halo.get(own, hi, bl, n2) + halo.diag(along_y, hi, 2, 0, n2)
        low = halo.get(theirs, hi, bl + 2 * n2, n2) + 0.0625 * halo.get(theirs, hi, bl + n2, n2) * near
        low = low + fl[pl.ds(0, n2), :]
        fl[pl.ds(0, n2, 2), :] = low
        fl[pl.ds(1, n2, 2), :] = low
        wide = times(fl[pl.ds(0, n1), :], doubling(128, 256))
        for k in range(2):
            near = halo.get(own, hi, bm + k * n1, n1) + halo.diag(along_y, hi, 1, k, n1)
            mid = halo.get(theirs, hi, bm + (4 + k) * n1, n1) + wide[:, cols(k)]
            mid = mid + 0.25 * halo.get(theirs, hi, bm + (2 + k) * n1, n1) * near
            fm[k, pl.ds(base, n1, 2), :] = mid
            fm[k, pl.ds(base + 1, n1, 2), :] = mid


def fine_kernel(r_v, d_v, s0, rep_m, fm, left_in, sxa, sxb, sya, syb, rxa, rxb, rya, ryb, rsa, rsb,
                p, im, sums, hy):
    halo = Halo((sxa, sxb), (sya, syb), None, (rxa, rxb), (rya, ryb), (rsa, rsb))
    twice = doubling(256, Z)

    def spread(i, carry):
        wide = times(take(rep_m, pl.ds(128 * i, 128)), twice).reshape(4, 1, Y, Z)
        wide = jnp.broadcast_to(wide, (4, 2, Y, Z)).reshape(8 * Y, Z)
        for k in range(4):
            p[k, pl.ds(8 * Y * i + Y, 8 * Y), :] = wide[:, cols(k)] + s0[k, pl.ds(8 * Y * i, 8 * Y), :]
        return carry

    lax.fori_loop(0, 8, spread, 0)
    for hi in range(2):
        for k in range(4):
            rows = pl.ds(Y + hi * (X - 1) * Y, Y)
            p[k, rows, :] = p[k, rows, :] + halo.get("sx", hi, XF + (4 + k) * Y, Y) * halo.get("rx", hi, XF + k * Y, Y)
    for hi in range(2):
        for k in range(4):
            rows = pl.ds(Y + hi * (Y - 1), X, Y)
            p[k, rows, :] = p[k, rows, :] + halo.get("sy", hi, (4 + k) * X, X) * halo.get("ry", hi, k * X, X)

    outer = times(take(fm, pl.ds(0, 2 * (X + Y))), twice)
    for (along_y, hi), base in zip(FACES, FACE_ROWS):
        n = X if along_y else Y
        theirs, own, bf = ("ry", "sy", 0) if along_y else ("rx", "sx", XF)
        for k in range(4):
            near = halo.get(own, hi, bf + k * n, n) + halo.diag(along_y, hi, 0, k, n)
            inv = halo.get(theirs, hi, bf + (4 + k) * n, n)
            fine = halo.get(theirs, hi, bf + (8 + k) * n, n) + inv * near + outer[base:base + n, cols(k)]
            fine = jnp.where(inv > 0.0, fine, 0.0)
            if along_y:
                hy[hi, :, cols(k)] = fine
            else:
                p[k, pl.ds(hi * (X + 1) * Y, Y), :] = fine

    def fold(v):
        v = (v[0:8] + v[8:16]) + (v[16:24] + v[24:32])
        return (v[:, cols(0)] + v[:, cols(1)]) + (v[:, cols(2)] + v[:, cols(3)])

    def image(i, carry):
        rows = pl.ds(Y * i, Y)
        c = take(p, pl.ds(Y * i + Y, Y))
        around = in_plane(c, hy[0, pl.ds(i, 1), :], hy[1, pl.ds(i, 1), :])
        around = around + (take(p, rows) + take(p, pl.ds(Y * i + 2 * Y, Y)))
        dd, rr = take(d_v, rows), take(r_v, rows)
        out = (6.0 + dd) * c - around
        im[rows, :] = out
        return tuple(t + fold(v) for t, v in zip(carry, (rr * c, c * out, rr, out, dd)))

    start = jnp.zeros((8, LANES), F32)
    totals = lax.fori_loop(0, X, image, (start,) * 5)
    totals = [jnp.sum(t) for t in totals] + [left_in[0:1, 0:1]]
    lane = iota((LANES, 8), 1)
    packed = jnp.zeros((LANES, 8), F32)
    for n, t in enumerate(totals):
        packed = jnp.where(lane == n, t, packed)
    sums[...] = packed


def final_kernel(every, r_v, d_v, p, im, update, residual):
    step = pl.program_id(0)
    gx, gy = lax.axis_index("gx"), lax.axis_index("gy")
    total = jnp.sum(every[...], axis=0, keepdims=True)
    lane8 = iota((1, 8), 1)
    rz, zq, res_sum, image_sum, coef_sum, left = [jnp.sum(jnp.where(lane8 == n, total, 0.0), axis=1, keepdims=True) for n in range(6)]
    shift = left / (coef_sum / 512.0 + 6.0 * 64.0 * 64.0 / 64.0)
    ones_sum = coef_sum + 6.0 * WHOLE * WHOLE
    alpha = (rz + shift * res_sum) / (zq + shift * (2.0 * image_sum + shift * ones_sum))
    scaled = alpha * shift
    row, lane = iota((Y, Z), 0), iota((Y, Z), 1)
    walls = jnp.where(lane == 0, 1.0, 0.0) + jnp.where(lane == Z - 1, 1.0, 0.0)
    walls = walls + jnp.where((row == 0) & (gy == 0), 1.0, 0.0)
    walls = walls + jnp.where((row == Y - 1) & (gy == DEVS_Y - 1), 1.0, 0.0)

    def plane(i, carry):
        x = step * CHUNK + i
        end = ((x == 0) & (gx == 0)) | ((x == X - 1) & (gx == DEVS_X - 1))
        rows = pl.ds(x * Y, Y)
        outside = walls + jnp.where(end, 1.0, 0.0)
        here = pl.ds(i * Y, Y)
        update[here, :] = alpha * take(p, pl.ds(x * Y + Y, Y)) + scaled
        residual[here, :] = take(r_v, rows) - alpha * im[rows, :] - scaled * (take(d_v, rows) + outside)
        return carry

    lax.fori_loop(0, CHUNK, plane, 0, unroll=2)


def f32(*shape):
    return jax.ShapeDtypeStruct(shape, F32)


def resident(*shape):
    return pltpu.VMEM(shape, F32)


def in_vmem(value):
    return pltpu.with_memory_space_constraint(value, pltpu.VMEM)


VM = pl.BlockSpec(memory_space=pltpu.VMEM)


def swap(value, axis, distance, offset):
    count = lax.axis_size(axis)
    pairs = []
    for i in range(count - distance):
        if (i // distance) % 2 == offset:
            pairs += [(i, i + distance), (i + distance, i)]
    return lax.ppermute(value, axis, pairs)


def body(right_side, diagonal):
    r = right_side.reshape(X * Y, Z)
    d = diagonal.reshape(X * Y, Z)
    vm = pltpu.VMEM
    hbm = pl.BlockSpec(memory_space=pl.ANY)
    r_v, d_v, g, inv, sxa, sxb, sma, smb, s1, s2 = pl.pallas_call(
        restrict_kernel,
        in_specs=[hbm, hbm],
        out_specs=[VM] * 10,
        out_shape=[resident(4, X * Y, LANES)] * 2 + [resident(4, (X + 2) * Y, LANES), resident(4, X * Y, LANES)]
        + [resident(XROWS, LANES)] * 2 + [resident(YB, LANES)] * 2 + [resident(2, 512, LANES), resident(128, 128)],
        scratch_shapes=[vm((2, 512, LANES), F32), vm((2, 512, LANES), F32),
                        vm((2, 544, LANES), F32), vm((2, 512, LANES), F32)] + [vm((128, 128), F32)] * 4
        + [pltpu.SemaphoreType.DMA((2, X // CHUNK, 4))],
        compiler_params=pltpu.CompilerParams(vmem_limit_bytes=12 * 2**20),
        name="restrict_all",
    )(pltpu.with_memory_space_constraint(r, pltpu.HBM), pltpu.with_memory_space_constraint(d, pltpu.HBM))

    rxa = swap(sxa, "gx", 1, 0)
    rxb = swap(sxb, "gx", 1, 1)
    s0, sya, syb = pl.pallas_call(
        smooth_kernel,
        in_specs=[VM] * 3,
        out_specs=[VM] * 3,
        out_shape=[resident(4, X * Y, LANES)] + [resident(768, LANES)] * 2,
        compiler_params=pltpu.CompilerParams(vmem_limit_bytes=4 * 2**20),
        cost_estimate=pl.CostEstimate(flops=COST, transcendentals=0, bytes_accessed=0),
        name="smooth_fine",
    )(in_vmem(r_v), in_vmem(g), in_vmem(inv))
    block, outa, outb = pl.pallas_call(
        pack_kernel,
        in_specs=[VM] * 5,
        out_specs=[VM] * 3,
        out_shape=[resident(96, LANES), resident(YROWS, LANES), resident(YROWS, LANES)],
        compiler_params=pltpu.CompilerParams(vmem_limit_bytes=2 * 2**20),
        name="pack_faces",
    )(in_vmem(sxa), rxa, rxb, in_vmem(sma), in_vmem(smb))
    r2a = swap(block, "gy", 2, 0)
    r2b = swap(block, "gy", 2, 1)
    rsa = swap(outa, "gy", 1, 0)
    rsb = swap(outb, "gy", 1, 1)
    rya = swap(sya, "gy", 1, 0)
    ryb = swap(syb, "gy", 1, 1)

    rep, faces, left = pl.pallas_call(
        coarse_kernel,
        in_specs=[VM] * 13,
        out_specs=[VM] * 3,
        out_shape=[resident(2, 1024, LANES), resident(2, 2 * (X + Y), LANES), resident(8, LANES)],
        scratch_shapes=[vm((20, 24, LANES), F32), vm((22, 24, LANES), F32), vm((22, 24, LANES), F32), vm((144, LANES), F32),
                        vm((128, 128), F32), vm((256, 128), F32), vm((2, 512, LANES), F32), vm((32, LANES), F32)],
        compiler_params=pltpu.CompilerParams(vmem_limit_bytes=8 * 2**20),
        cost_estimate=pl.CostEstimate(flops=COST, transcendentals=0, bytes_accessed=0),
        name="solve_coarse",
    )(in_vmem(s1), in_vmem(s2), in_vmem(sxa), in_vmem(sxb), in_vmem(sma), in_vmem(smb), in_vmem(block),
      rxa, rxb, rsa, rsb, r2a, r2b)
    p, im, sums = pl.pallas_call(
        fine_kernel,
        in_specs=[VM] * 16,
        out_specs=[VM] * 3,
        out_shape=[resident(4, (X + 2) * Y, LANES), resident(X * Y, Z), f32(LANES, 8)],
        scratch_shapes=[vm((2, X, Z), F32)],
        compiler_params=pltpu.CompilerParams(vmem_limit_bytes=8 * 2**20),
        name="solve_fine",
    )(in_vmem(r_v), in_vmem(d_v), in_vmem(s0), in_vmem(rep), in_vmem(faces), in_vmem(left),
      in_vmem(sxa), in_vmem(sxb), in_vmem(sya), in_vmem(syb), rxa, rxb, rya, ryb, rsa, rsb)

    every = lax.all_to_all(sums, ("gx", "gy"), 0, 0, tiled=True)
    blocks = pl.BlockSpec((CHUNK * Y, Z), lambda i: (i, 0))
    update, residual = pl.pallas_call(
        final_kernel,
        grid=(X // CHUNK,),
        in_specs=[VM] * 5,
        out_specs=[blocks, blocks],
        out_shape=[f32(X * Y, Z), f32(X * Y, Z)],
        compiler_params=pltpu.CompilerParams(vmem_limit_bytes=8 * 2**20),
        name="scale_outputs",
    )(every, in_vmem(r_v), in_vmem(d_v), in_vmem(p), in_vmem(im))
    return update.reshape(X, Y, Z), residual.reshape(X, Y, Z)


def solution(mesh):
    return jax.shard_map(
        body,
        mesh=mesh,
        in_specs=(P("gx", "gy", None), P("gx", "gy", None)),
        out_specs=(P("gx", "gy", None), P("gx", "gy", None)),
        check_vma=False,
    )
```

```python
import jax
import jax.numpy as jnp
from jax import lax
from jax.experimental import pallas as pl
from jax.experimental.pallas import tpu as pltpu
from jax.sharding import PartitionSpec as P

F32 = jnp.float32
BF16 = jnp.bfloat16

X, Y, Z = 64, 32, 512
DEVS_X, DEVS_Y = 8, 16
WHOLE = 512
LANES = 128
COST = 20_000_000
CHUNK = 8

XF, XM, XL, XB, XROWS = 0, 384, 480, 504, 536
YF, YM, YL, YB, YC, YROWS = 0, 256, 320, 336, 432, 448
OM, OL, OROWS = 0, 128, 160


def iota(shape, axis):
    return lax.broadcasted_iota(jnp.int32, shape, axis)


def halving(depth, cols, offset=0):
    coarse = lax.shift_right_logical(iota((depth, cols), 0), 1) + offset
    return jnp.where(coarse == iota((depth, cols), 1), 0.125, 0.0).astype(BF16)


def doubling(depth, cols):
    coarse = lax.shift_right_logical(iota((depth, cols), 1), 1)
    return jnp.where(coarse == iota((depth, cols), 0), 1.0, 0.0).astype(BF16)


def times(value, table):
    high = value.astype(BF16)
    low = (value - high.astype(F32)).astype(BF16)
    return jnp.dot(high, table, preferred_element_type=F32) + jnp.dot(low, table, preferred_element_type=F32)


def in_plane(c, top, bottom):
    rows, lanes = c.shape
    row, lane = iota(c.shape, 0), iota(c.shape, 1)
    up = jnp.where(row == 0, top, pltpu.roll(c, 1, 0))
    down = jnp.where(row == rows - 1, bottom, pltpu.roll(c, rows - 1, 0))
    left = jnp.where(lane == 0, 0.0, pltpu.roll(c, 1, 1))
    right = jnp.where(lane == lanes - 1, 0.0, pltpu.roll(c, lanes - 1, 1))
    return (up + down) + (left + right)


def cols(k):
    return slice(LANES * k, LANES * (k + 1))


def take(ref, rows):
    return jnp.concatenate([ref[k, rows, :] for k in range(ref.shape[0])], axis=1)


def put(ref, rows, value):
    for k in range(ref.shape[0]):
        ref[k, rows, :] = value[:, cols(k)]


def send(parity, first, second, rows, low, high):
    first[rows, :] = jnp.where(parity == 0, high, low)
    second[rows, :] = jnp.where(parity == 0, low, high)


def parities():
    gx, gy = lax.axis_index("gx"), lax.axis_index("gy")
    return gx % 2, gy % 2, (gy // 2) % 2


def restrict_kernel(r_hbm, d_hbm, r_v, d_v, g_s, i_s, sxa, sxb, gya, gyb, om, s1, s2,
                    rm, cm, gm, im, rl, cl, gl, il, sems):
    px, py, _ = parities()

    def copies(c):
        rows = pl.ds(c * CHUNK * Y, CHUNK * Y)
        for n, (src, dst) in enumerate(((r_hbm, r_v), (d_hbm, d_v))):
            for k in range(4):
                yield pltpu.make_async_copy(src.at[rows, pl.ds(LANES * k, LANES)], dst.at[k, rows], sems.at[n, c, k])

    for c in range(X // CHUNK):
        for one in copies(c):
            one.start()

    for k in range(4):
        g_s[k, pl.ds(0, Y), :] = jnp.zeros((Y, LANES), F32)
        g_s[k, pl.ds((X + 1) * Y, Y), :] = jnp.zeros((Y, LANES), F32)
    for k in range(2):
        gm[k, pl.ds(0, 16), :] = jnp.zeros((16, LANES), F32)
        gm[k, pl.ds(33 * 16, 16), :] = jnp.zeros((16, LANES), F32)
    half = halving(512, 256)

    def load(c, carry):
        for one in copies(c):
            one.wait()
        base = c * CHUNK * Y

        def plane(i, carry):
            rows = pl.ds(base + i * Y, Y)
            inv = 0.8 / (6.0 + take(d_v, rows))
            put(i_s, rows, inv)
            put(g_s, pl.ds(base + (i + 1) * Y, Y), inv * take(r_v, rows))
            return carry

        lax.fori_loop(0, CHUNK, plane, 0)
        n = CHUNK * Y // 2
        for src, dst in ((r_v, rm), (d_v, cm)):
            pairs = jnp.concatenate(
                [src[k, pl.ds(base, n, 2), :] + src[k, pl.ds(base + 1, n, 2), :] for k in range(4)], axis=1)
            pairs = pairs.reshape(CHUNK // 2, 2, 16, Z)
            pairs = (pairs[:, 0] + pairs[:, 1]).reshape(CHUNK // 2 * 16, Z)
            put(dst, pl.ds(c * (CHUNK // 2 * 16), CHUNK // 2 * 16), times(pairs, half))
        return carry

    lax.fori_loop(0, X // CHUNK, load, 0)

    half = halving(256, 128)
    for src, dst in ((rm, rl), (cm, cl)):
        pairs = jnp.concatenate([src[k, pl.ds(0, 256, 2), :] + src[k, pl.ds(1, 256, 2), :] for k in range(2)], axis=1)
        pairs = pairs.reshape(16, 2, 8, 256)
        pairs = (pairs[:, 0] + pairs[:, 1]).reshape(128, 256)
        dst[...] = times(pairs, half)
    packed = 0.0
    for src, offset in ((rl, 0), (cl, 64)):
        quad = [sum(src[pl.ds(8 * f + 2 * j + e, 8, 16), :] for e in range(2) for f in range(2)) for j in range(4)]
        packed = packed + times(jnp.concatenate(quad, axis=0), halving(128, 128, offset))
    sxa[pl.ds(XB, 32), :] = packed
    sxb[pl.ds(XB, 32), :] = packed

    inv = 0.8 / (0.09375 * 4.0 + cl[...])
    il[...] = inv
    gl[...] = inv * rl[...]
    for i in range(16):
        rows = pl.ds(8 * i, 8)
        c = gl[rows, :]
        total = in_plane(c, 0.0, 0.0)
        if i > 0:
            total = total + gl[pl.ds(8 * i - 8, 8), :]
        if i < 15:
            total = total + gl[pl.ds(8 * i + 8, 8), :]
        s2[rows, :] = il[rows, :] * (1.2 * rl[rows, :] + 0.0625 * total)

    def guess(i, carry):
        rows = pl.ds(64 * i, 64)
        inv = 0.8 / (1.5 + take(cm, rows))
        put(im, rows, inv)
        put(gm, pl.ds(64 * i + 16, 64), inv * take(rm, rows))
        return carry

    lax.fori_loop(0, 8, guess, 0)

    def middle(i, carry):
        rows = pl.ds(16 * i, 16)
        c = take(gm, pl.ds(16 * i + 16, 16))
        total = in_plane(c, 0.0, 0.0) + (take(gm, rows) + take(gm, pl.ds(16 * i + 32, 16)))
        put(s1, rows, take(im, rows) * (1.2 * take(rm, rows) + 0.25 * total))
        return carry

    lax.fori_loop(0, 32, middle, 0, unroll=4)

    ends = []
    for i, near in ((0, 1), (X - 1, X - 2)):
        rows = pl.ds(Y * i, Y)
        g, inv = take(g_s, pl.ds(Y * i + Y, Y)), take(i_s, rows)
        total = in_plane(g, 0.0, 0.0) + take(g_s, pl.ds(Y * near + Y, Y))
        ends.append((g, inv, inv * (1.2 * take(r_v, rows) + total)))
    for a in range(3):
        for k in range(4):
            send(px, sxa, sxb, pl.ds(XF + (4 * a + k) * Y, Y), ends[0][a][:, cols(k)], ends[1][a][:, cols(k)])
    for a, (ref, pad) in enumerate(((gm, 16), (im, 0), (s1, 0))):
        for k in range(2):
            send(px, sxa, sxb, pl.ds(XM + (2 * a + k) * 16, 16),
                 ref[k, pl.ds(pad, 16), :], ref[k, pl.ds(pad + 31 * 16, 16), :])
            low, high = ref[k, pl.ds(pad, 32, 16), :], ref[k, pl.ds(pad + 15, 32, 16), :]
            if a == 0:
                send(py, gya, gyb, pl.ds(YM + k * 32, 32), low, high)
            else:
                om[0, pl.ds(OM + (2 * a - 2 + k) * 32, 32), :] = low
                om[1, pl.ds(OM + (2 * a - 2 + k) * 32, 32), :] = high
    for a, ref in enumerate((gl, il, s2)):
        send(px, sxa, sxb, pl.ds(XL + a * 8, 8), ref[pl.ds(0, 8), :], ref[pl.ds(15 * 8, 8), :])
        low, high = ref[pl.ds(0, 16, 8), :], ref[pl.ds(7, 16, 8), :]
        if a == 0:
            send(py, gya, gyb, pl.ds(YL, 16), low, high)
        else:
            om[0, pl.ds(OL + (a - 1) * 16, 16), :] = low
            om[1, pl.ds(OL + (a - 1) * 16, 16), :] = high
    for k in range(4):
        send(py, gya, gyb, pl.ds(YF + k * X, X), g_s[k, pl.ds(Y, X, Y), :], g_s[k, pl.ds(2 * Y - 1, X, Y), :])


def smooth_kernel(r_v, g_s, i_s, s0, of):
    def fine(i, carry):
        rows = pl.ds(Y * i, Y)
        c = take(g_s, pl.ds(Y * i + Y, Y))
        total = in_plane(c, 0.0, 0.0) + (take(g_s, rows) + take(g_s, pl.ds(Y * i + 2 * Y, Y)))
        put(s0, rows, take(i_s, rows) * (1.2 * take(r_v, rows) + total))
        return carry

    lax.fori_loop(0, X, fine, 0, unroll=8)
    for a, ref in enumerate((i_s, s0)):
        for k in range(4):
            for hi in range(2):
                of[hi, pl.ds((4 * a + k) * X, X), :] = ref[k, pl.ds(hi * (Y - 1), X, Y), :]


def pick(slot, first, second, rows):
    return jnp.where(slot == 0, first[rows, :], second[rows, :])


class Halo:
    def __init__(self, **pairs):
        self.px, self.py, _ = parities()
        self.pairs = pairs

    def get(self, name, hi, start, n):
        parity = self.px if name in ("sx", "rx") else self.py
        return pick(parity if hi else 1 - parity, *self.pairs[name], pl.ds(start, n))

    def diag(self, hi, level, k, rows):
        return ends(rows, *[self.get("rs", yhi, YC + 7 * hi + (0, 4, 6)[level] + k, 1) for yhi in range(2)])


def ends(rows, first, last):
    row = iota((rows, LANES), 0)
    return jnp.where(row == 0, first, jnp.where(row == rows - 1, last, 0.0))


def pack_kernel(sxa, rxa, rxb, rga, rgb, of, om, block, outa, outb):
    halo = Halo(rx=(rxa, rxb), rg=(rga, rgb))
    for j in range(4):
        rows = pl.ds(XB + 8 * j, 8)
        block[pl.ds(24 * j, 8), :] = halo.get("rx", 0, XB + 8 * j, 8)
        block[pl.ds(24 * j + 8, 8), :] = sxa[rows, :]
        block[pl.ds(24 * j + 16, 8), :] = halo.get("rx", 1, XB + 8 * j, 8)
    for out in (outa, outb):
        out[pl.ds(YB, 96), :] = block[...]
    sides = []
    for hi in range(2):
        parts = []

        def layer(scale, own, inv, field, n, rows, base, width, k):
            beside = [halo.get("rx", x, base + k * width + hi * (width - 1), 1) for x in range(2)]
            near = halo.get("rg", hi, rows + k * n, n) + ends(n, *beside)
            parts.append(own[hi, pl.ds(field + k * n, n), :] + scale * own[hi, pl.ds(inv + k * n, n), :] * near)

        for k in range(4):
            layer(1.0, of, 0, 4 * X, X, YF, XF, Y, k)
        for k in range(2):
            layer(0.25, om, OM, OM + 64, 32, YM, XM, 16, k)
        layer(0.0625, om, OL, OL + 16, 16, YL, XL, 8, 0)
        corner = []
        for xhi in range(2):
            for base, n, ks in ((XF, Y, 4), (XM, 16, 2), (XL, 8, 1)):
                for k in range(ks):
                    corner.append(halo.get("rx", xhi, base + k * n + hi * (n - 1), 1))
        corner.append(jnp.zeros((2, LANES), F32))
        sides.append((jnp.concatenate(parts, axis=0), jnp.concatenate(corner, axis=0)))
    (low, low_corner), (high, high_corner) = sides
    send(halo.py, outa, outb, pl.ds(0, YB), low, high)
    send(halo.py, outa, outb, pl.ds(YC, 16), low_corner, high_corner)


FACES = ((False, 0), (False, 1), (True, 0), (True, 1))
FACE_ROWS = (0, Y, 2 * Y, 2 * Y + X)


def coarse_kernel(s1, s2, sxa, sxb, om, block, rxa, rxb, rga, rgb, rsa, rsb, r2a, r2b,
                  rep_m, fm, left_out,
                  bs, ga, gb, sz, low_s, rep_l, mid_s, fl):
    px, py, qy = parities()
    halo = Halo(sx=(sxa, sxb), rx=(rxa, rxb), rg=(rga, rgb), rs=(rsa, rsb))

    ysel = (lambda hi: py if hi else 1 - py)
    q = (lambda hi: qy if hi else 1 - qy)
    low2, low1 = pick(q(0), r2a, r2b, slice(None)), pick(ysel(0), rsa, rsb, pl.ds(YB, 96))
    high1, high2 = pick(ysel(1), rsa, rsb, pl.ds(YB, 96)), pick(q(1), r2a, r2b, slice(None))
    for n, part in enumerate((low2, low1, block[...], high1, high2)):
        bs[pl.ds(4 * n, 4)] = part.reshape(4, 24, LANES)
    shape = (20, 24, LANES)
    live = iota(shape, 2) < 64
    both = bs[...]
    res = jnp.where(live, both, 0.0)
    coef = jnp.where(live, pltpu.roll(both, 64, 2), 0.0)
    inv = jnp.where(coef > 0.0, 0.8 / (0.09375 + coef), 0.0)
    zero = jnp.zeros((24, LANES), F32)
    for ref in (ga, gb):
        ref[0] = zero
        ref[21] = zero

    def around(ref):
        c = ref[pl.ds(1, 20)]
        total = ref[pl.ds(0, 20)] + ref[pl.ds(2, 20)]
        total = total + (pltpu.roll(c, 1, 1) + pltpu.roll(c, 23, 1))
        return c, total + (pltpu.roll(c, 1, 2) + pltpu.roll(c, LANES - 1, 2))

    ga[pl.ds(1, 20)] = inv * res
    bs[...] = inv
    now, new = ga, gb
    for sweep in range(7):
        c, total = around(now)
        new[pl.ds(1, 20)] = c + bs[...] * (res - ((0.09375 + coef) * c - 0.015625 * total))
        now, new = new, now
    c, total = around(now)
    left = res - ((0.09375 + coef) * c - 0.015625 * total)
    leftover = jnp.sum(jnp.where(live[8:12, 8:16], left[8:12, 8:16], 0.0))
    sz[...] = times(now[pl.ds(8, 6)].reshape(144, LANES), doubling(LANES, LANES))

    left_out[...] = jnp.full((8, LANES), leftover, F32)

    for j in range(4):
        for e in range(2):
            for f in range(2):
                low_s[pl.ds(8 * f + 2 * j + e, 8, 16), :] = sz[pl.ds(24 * (j + 1) + 8, 8), :]
    low_s[...] = low_s[...] + s2[...]
    for hi in range(2):
        rows = pl.ds(hi * 120, 8)
        low_s[rows, :] = low_s[rows, :] + 0.0625 * halo.get("sx", hi, XL + 8, 8) * halo.get("rx", hi, XL, 8)
    for hi in range(2):
        rows = pl.ds(hi * 7, 16, 8)
        low_s[rows, :] = low_s[rows, :] + 0.0625 * om[hi, pl.ds(OL, 16), :] * halo.get("rg", hi, YL, 16)

    rep_l[pl.ds(0, 128, 2), :] = low_s[...]
    rep_l[pl.ds(1, 128, 2), :] = low_s[...]
    wide = times(rep_l[...], doubling(128, 256)).reshape(16, 1, 16, 256)
    wide = jnp.broadcast_to(wide, (16, 2, 16, 256)).reshape(512, 256)
    for k in range(2):
        mid_s[k] = wide[:, cols(k)] + s1[k]
    for hi in range(2):
        for k in range(2):
            rows = pl.ds(hi * 496, 16)
            mid_s[k, rows, :] = mid_s[k, rows, :] + (
                0.25 * halo.get("sx", hi, XM + 32 + 16 * k, 16) * halo.get("rx", hi, XM + 16 * k, 16))
    for hi in range(2):
        for k in range(2):
            rows = pl.ds(hi * 15, 32, 16)
            mid_s[k, rows, :] = mid_s[k, rows, :] + (
                0.25 * om[hi, pl.ds(OM + 32 * k, 32), :] * halo.get("rg", hi, YM + 32 * k, 32))

    for k in range(2):
        rep_m[k, pl.ds(0, 512, 2), :] = mid_s[k]
        rep_m[k, pl.ds(1, 512, 2), :] = mid_s[k]
    for (along_y, hi), base in zip(FACES, FACE_ROWS):
        n = X if along_y else Y
        n2, n1 = n // 4, n // 2
        if along_y:
            top = sz[pl.ds(120 * hi + 8, 8), :]
        else:
            top = sz[pl.ds(24 + (16 if hi else 7), 4, 24), :]
        fl[pl.ds(0, n2 // 2, 2), :] = top
        fl[pl.ds(1, n2 // 2, 2), :] = top
        if along_y:
            low = halo.get("rs", hi, YL, n2)
        else:
            near = halo.get("sx", hi, XL, n2) + halo.diag(hi, 2, 0, n2)
            low = halo.get("rx", hi, XL + 2 * n2, n2) + 0.0625 * halo.get("rx", hi, XL + n2, n2) * near
        low = low + fl[pl.ds(0, n2), :]
        fl[pl.ds(0, n2, 2), :] = low
        fl[pl.ds(1, n2, 2), :] = low
        wide = times(fl[pl.ds(0, n1), :], doubling(128, 256))
        for k in range(2):
            if along_y:
                mid = halo.get("rs", hi, YM + k * n1, n1)
            else:
                near = halo.get("sx", hi, XM + k * n1, n1) + halo.diag(hi, 1, k, n1)
                mid = halo.get("rx", hi, XM + (4 + k) * n1, n1) + 0.25 * halo.get("rx", hi, XM + (2 + k) * n1, n1) * near
            mid = mid + wide[:, cols(k)]
            fm[k, pl.ds(base, n1, 2), :] = mid
            fm[k, pl.ds(base + 1, n1, 2), :] = mid


def fine_kernel(r_v, d_v, s0, rep_m, fm, left_in, sxa, sxb, of, rxa, rxb, rga, rgb, rsa, rsb,
                p, im, sums, hy):
    halo = Halo(sx=(sxa, sxb), rx=(rxa, rxb), rg=(rga, rgb), rs=(rsa, rsb))
    gy = lax.axis_index("gy")
    twice = doubling(256, Z)

    def spread(i, carry):
        wide = times(take(rep_m, pl.ds(128 * i, 128)), twice).reshape(4, 1, Y, Z)
        wide = jnp.broadcast_to(wide, (4, 2, Y, Z)).reshape(8 * Y, Z)
        for k in range(4):
            p[k, pl.ds(8 * Y * i + Y, 8 * Y), :] = wide[:, cols(k)] + s0[k, pl.ds(8 * Y * i, 8 * Y), :]
        return carry

    lax.fori_loop(0, 8, spread, 0, unroll=2)
    for hi in range(2):
        for k in range(4):
            rows = pl.ds(Y + hi * (X - 1) * Y, Y)
            p[k, rows, :] = p[k, rows, :] + halo.get("sx", hi, XF + (4 + k) * Y, Y) * halo.get("rx", hi, XF + k * Y, Y)
    for hi in range(2):
        for k in range(4):
            rows = pl.ds(Y + hi * (Y - 1), X, Y)
            p[k, rows, :] = p[k, rows, :] + of[hi, pl.ds(k * X, X), :] * halo.get("rg", hi, YF + k * X, X)

    outer = times(take(fm, pl.ds(0, 2 * (X + Y))), twice)
    for (along_y, hi), base in zip(FACES, FACE_ROWS):
        n = X if along_y else Y
        for k in range(4):
            above = outer[base:base + n, cols(k)]
            if along_y:
                wall = gy == (DEVS_Y - 1 if hi else 0)
                hy[hi, :, cols(k)] = jnp.where(wall, 0.0, halo.get("rs", hi, YF + k * n, n) + above)
            else:
                near = halo.get("sx", hi, XF + k * n, n) + halo.diag(hi, 0, k, n)
                inv = halo.get("rx", hi, XF + (4 + k) * n, n)
                fine = halo.get("rx", hi, XF + (8 + k) * n, n) + inv * near + above
                p[k, pl.ds(hi * (X + 1) * Y, Y), :] = jnp.where(inv > 0.0, fine, 0.0)

    def fold(v):
        v = (v[0:8] + v[8:16]) + (v[16:24] + v[24:32])
        return (v[:, cols(0)] + v[:, cols(1)]) + (v[:, cols(2)] + v[:, cols(3)])

    def image(i, carry):
        rows = pl.ds(Y * i, Y)
        c = take(p, pl.ds(Y * i + Y, Y))
        around = in_plane(c, hy[0, pl.ds(i, 1), :], hy[1, pl.ds(i, 1), :])
        around = around + (take(p, rows) + take(p, pl.ds(Y * i + 2 * Y, Y)))
        dd, rr = take(d_v, rows), take(r_v, rows)
        out = (6.0 + dd) * c - around
        im[rows, :] = out
        return tuple(t + fold(v) for t, v in zip(carry, (rr * c, c * out, rr, out, dd)))

    start = jnp.zeros((8, LANES), F32)
    totals = lax.fori_loop(0, X, image, (start,) * 5, unroll=8)
    totals = [jnp.sum(t) for t in totals] + [left_in[0:1, 0:1]]
    lane = iota((LANES, 8), 1)
    packed = jnp.zeros((LANES, 8), F32)
    for n, t in enumerate(totals):
        packed = jnp.where(lane == n, t, packed)
    sums[...] = packed


def final_kernel(every, r_v, d_v, p, im, update, residual):
    step = pl.program_id(0)
    gx, gy = lax.axis_index("gx"), lax.axis_index("gy")
    total = jnp.sum(every[...], axis=0, keepdims=True)
    lane8 = iota((1, 8), 1)
    rz, zq, res_sum, image_sum, coef_sum, left = [jnp.sum(jnp.where(lane8 == n, total, 0.0), axis=1, keepdims=True) for n in range(6)]
    shift = left / (coef_sum / 512.0 + 6.0 * 64.0 * 64.0 / 64.0)
    ones_sum = coef_sum + 6.0 * WHOLE * WHOLE
    alpha = (rz + shift * res_sum) / (zq + shift * (2.0 * image_sum + shift * ones_sum))
    scaled = alpha * shift
    row, lane = iota((Y, Z), 0), iota((Y, Z), 1)
    walls = jnp.where(lane == 0, 1.0, 0.0) + jnp.where(lane == Z - 1, 1.0, 0.0)
    walls = walls + jnp.where((row == 0) & (gy == 0), 1.0, 0.0)
    walls = walls + jnp.where((row == Y - 1) & (gy == DEVS_Y - 1), 1.0, 0.0)

    def plane(i, carry):
        x = step * CHUNK + i
        end = ((x == 0) & (gx == 0)) | ((x == X - 1) & (gx == DEVS_X - 1))
        rows = pl.ds(x * Y, Y)
        outside = walls + jnp.where(end, 1.0, 0.0)
        here = pl.ds(i * Y, Y)
        update[here, :] = alpha * take(p, pl.ds(x * Y + Y, Y)) + scaled
        residual[here, :] = take(r_v, rows) - alpha * im[rows, :] - scaled * (take(d_v, rows) + outside)
        return carry

    lax.fori_loop(0, CHUNK, plane, 0, unroll=2)


def f32(*shape):
    return jax.ShapeDtypeStruct(shape, F32)


def resident(*shape):
    return pltpu.VMEM(shape, F32)


def in_vmem(value):
    return pltpu.with_memory_space_constraint(value, pltpu.VMEM)


VM = pl.BlockSpec(memory_space=pltpu.VMEM)


def swap(value, axis, distance, offset):
    count = lax.axis_size(axis)
    pairs = []
    for i in range(count - distance):
        if (i // distance) % 2 == offset:
            pairs += [(i, i + distance), (i + distance, i)]
    return lax.ppermute(value, axis, pairs)


def body(right_side, diagonal):
    r = right_side.reshape(X * Y, Z)
    d = diagonal.reshape(X * Y, Z)
    vm = pltpu.VMEM
    hbm = pl.BlockSpec(memory_space=pl.ANY)
    r_v, d_v, g, inv, sxa, sxb, gya, gyb, om, s1, s2 = pl.pallas_call(
        restrict_kernel,
        in_specs=[hbm, hbm],
        out_specs=[VM] * 11,
        out_shape=[resident(4, X * Y, LANES)] * 2 + [resident(4, (X + 2) * Y, LANES), resident(4, X * Y, LANES)]
        + [resident(XROWS, LANES)] * 2 + [resident(YB, LANES)] * 2 + [resident(2, OROWS, LANES)]
        + [resident(2, 512, LANES), resident(128, 128)],
        scratch_shapes=[vm((2, 512, LANES), F32), vm((2, 512, LANES), F32),
                        vm((2, 544, LANES), F32), vm((2, 512, LANES), F32)] + [vm((128, 128), F32)] * 4
        + [pltpu.SemaphoreType.DMA((2, X // CHUNK, 4))],
        compiler_params=pltpu.CompilerParams(vmem_limit_bytes=12 * 2**20),
        name="restrict_all",
    )(pltpu.with_memory_space_constraint(r, pltpu.HBM), pltpu.with_memory_space_constraint(d, pltpu.HBM))

    rxa = swap(sxa, "gx", 1, 0)
    rxb = swap(sxb, "gx", 1, 1)
    rga = swap(gya, "gy", 1, 0)
    rgb = swap(gyb, "gy", 1, 1)
    s0, of = pl.pallas_call(
        smooth_kernel,
        in_specs=[VM] * 3,
        out_specs=[VM] * 2,
        out_shape=[resident(4, X * Y, LANES), resident(2, 8 * X, LANES)],
        compiler_params=pltpu.CompilerParams(vmem_limit_bytes=4 * 2**20),
        cost_estimate=pl.CostEstimate(flops=COST, transcendentals=0, bytes_accessed=0),
        name="smooth_fine",
    )(in_vmem(r_v), in_vmem(g), in_vmem(inv))
    block, outa, outb = pl.pallas_call(
        pack_kernel,
        in_specs=[VM] * 7,
        out_specs=[VM] * 3,
        out_shape=[resident(96, LANES)] + [resident(YROWS, LANES)] * 2,
        compiler_params=pltpu.CompilerParams(vmem_limit_bytes=2 * 2**20),
        name="pack_faces",
    )(in_vmem(sxa), rxa, rxb, rga, rgb, in_vmem(of), in_vmem(om))
    r2a = swap(block, "gy", 2, 0)
    r2b = swap(block, "gy", 2, 1)
    rsa = swap(outa, "gy", 1, 0)
    rsb = swap(outb, "gy", 1, 1)

    rep, faces, left = pl.pallas_call(
        coarse_kernel,
        in_specs=[VM] * 14,
        out_specs=[VM] * 3,
        out_shape=[resident(2, 1024, LANES), resident(2, 2 * (X + Y), LANES), resident(8, LANES)],
        scratch_shapes=[vm((20, 24, LANES), F32), vm((22, 24, LANES), F32), vm((22, 24, LANES), F32), vm((144, LANES), F32),
                        vm((128, 128), F32), vm((256, 128), F32), vm((2, 512, LANES), F32), vm((32, LANES), F32)],
        compiler_params=pltpu.CompilerParams(vmem_limit_bytes=8 * 2**20),
        cost_estimate=pl.CostEstimate(flops=COST, transcendentals=0, bytes_accessed=0),
        name="solve_coarse",
    )(in_vmem(s1), in_vmem(s2), in_vmem(sxa), in_vmem(sxb), in_vmem(om), in_vmem(block),
      rxa, rxb, rga, rgb, rsa, rsb, r2a, r2b)
    p, im, sums = pl.pallas_call(
        fine_kernel,
        in_specs=[VM] * 15,
        out_specs=[VM] * 3,
        out_shape=[resident(4, (X + 2) * Y, LANES), resident(X * Y, Z), f32(LANES, 8)],
        scratch_shapes=[vm((2, X, Z), F32)],
        compiler_params=pltpu.CompilerParams(vmem_limit_bytes=8 * 2**20),
        name="solve_fine",
    )(in_vmem(r_v), in_vmem(d_v), in_vmem(s0), in_vmem(rep), in_vmem(faces), in_vmem(left),
      in_vmem(sxa), in_vmem(sxb), in_vmem(of), rxa, rxb, rga, rgb, rsa, rsb)

    every = lax.all_to_all(sums, ("gx", "gy"), 0, 0, tiled=True)
    blocks = pl.BlockSpec((CHUNK * Y, Z), lambda i: (i, 0))
    update, residual = pl.pallas_call(
        final_kernel,
        grid=(X // CHUNK,),
        in_specs=[VM] * 5,
        out_specs=[blocks, blocks],
        out_shape=[f32(X * Y, Z), f32(X * Y, Z)],
        compiler_params=pltpu.CompilerParams(vmem_limit_bytes=8 * 2**20),
        name="scale_outputs",
    )(every, in_vmem(r_v), in_vmem(d_v), in_vmem(p), in_vmem(im))
    return update.reshape(X, Y, Z), residual.reshape(X, Y, Z)


def solution(mesh):
    return jax.shard_map(
        body,
        mesh=mesh,
        in_specs=(P("gx", "gy", None), P("gx", "gy", None)),
        out_specs=(P("gx", "gy", None), P("gx", "gy", None)),
        check_vma=False,
    )
```

```python
import jax
import jax.numpy as jnp
from jax import lax
from jax.experimental import pallas as pl
from jax.experimental.pallas import tpu as pltpu
from jax.sharding import PartitionSpec as P


F32 = jnp.float32
BF16 = jnp.bfloat16

X, Y, Z = 64, 32, 512
DEVS_X, DEVS_Y = 8, 16
WHOLE = 512
LANES = 128
COST = 20_000_000
CHUNK = 8

XF, XM, XL, XB, XC, XROWS = 0, 384, 480, 504, 664, 680
YF, YM, YL, YB, YROWS = 0, 256, 448, 496, 528
ZROWS = 512
SCALE = (1.0, 0.25, 0.0625)


def iota(shape, axis):
    return lax.broadcasted_iota(jnp.int32, shape, axis)


def halving(depth, cols, offset=0):
    coarse = lax.shift_right_logical(iota((depth, cols), 0), 1) + offset
    return jnp.where(coarse == iota((depth, cols), 1), 0.125, 0.0).astype(BF16)


def doubling(depth, cols):
    coarse = lax.shift_right_logical(iota((depth, cols), 1), 1)
    return jnp.where(coarse == iota((depth, cols), 0), 1.0, 0.0).astype(BF16)


def times(value, table):
    high = value.astype(BF16)
    low = (value - high.astype(F32)).astype(BF16)
    return jnp.dot(high, table, preferred_element_type=F32) + jnp.dot(low, table, preferred_element_type=F32)


def in_plane(c, top, bottom):
    rows, lanes = c.shape
    row, lane = iota(c.shape, 0), iota(c.shape, 1)
    up = jnp.where(row == 0, top, pltpu.roll(c, 1, 0))
    down = jnp.where(row == rows - 1, bottom, pltpu.roll(c, rows - 1, 0))
    left = jnp.where(lane == 0, 0.0, pltpu.roll(c, 1, 1))
    right = jnp.where(lane == lanes - 1, 0.0, pltpu.roll(c, lanes - 1, 1))
    return (up + down) + (left + right)


def cols(k):
    return slice(LANES * k, LANES * (k + 1))


def take(ref, rows):
    return jnp.concatenate([ref[k, rows, :] for k in range(ref.shape[0])], axis=1)


def put(ref, rows, value):
    for k in range(ref.shape[0]):
        ref[k, rows, :] = value[:, cols(k)]


def fold(v):
    v = (v[0:8] + v[8:16]) + (v[16:24] + v[24:32])
    return (v[:, cols(0)] + v[:, cols(1)]) + (v[:, cols(2)] + v[:, cols(3)])


def send(parity, first, second, rows, low, high):
    first[rows, :] = jnp.where(parity == 0, high, low)
    second[rows, :] = jnp.where(parity == 0, low, high)


def parities():
    gx, gy = lax.axis_index("gx"), lax.axis_index("gy")
    return gx % 2, gy % 2, (gy // 2) % 2


def restrict_kernel(r_hbm, d_hbm, r_v, d_v, g_s, i_s, fx, sya, syb, sza, szb, core, rm, gm, im, s2, part,
                    cm, rl, cl, gl, il, sems):
    _, py, _ = parities()

    def copies(c):
        rows = pl.ds(c * CHUNK * Y, CHUNK * Y)
        for n, (src, dst) in enumerate(((r_hbm, r_v), (d_hbm, d_v))):
            for k in range(4):
                yield pltpu.make_async_copy(src.at[rows, pl.ds(LANES * k, LANES)], dst.at[k, rows], sems.at[n, c, k])

    for c in range(X // CHUNK):
        for one in copies(c):
            one.start()

    for k in range(4):
        g_s[k, pl.ds(0, Y), :] = jnp.zeros((Y, LANES), F32)
        g_s[k, pl.ds((X + 1) * Y, Y), :] = jnp.zeros((Y, LANES), F32)
    for k in range(2):
        gm[k, pl.ds(0, 16), :] = jnp.zeros((16, LANES), F32)
        gm[k, pl.ds(33 * 16, 16), :] = jnp.zeros((16, LANES), F32)
    half = halving(512, 256)

    def load(c, carry):
        for one in copies(c):
            one.wait()
        base = c * CHUNK * Y

        def plane(i, carry):
            rows = pl.ds(base + i * Y, Y)
            dd, rr = take(d_v, rows), take(r_v, rows)
            inv = 0.8 / (6.0 + dd)
            put(i_s, rows, inv)
            put(g_s, pl.ds(base + (i + 1) * Y, Y), inv * rr)
            return carry[0] + fold(rr), carry[1] + fold(dd)

        carry = lax.fori_loop(0, CHUNK, plane, carry)
        n = CHUNK * Y // 2
        for src, dst in ((r_v, rm), (d_v, cm)):
            pairs = jnp.concatenate(
                [src[k, pl.ds(base, n, 2), :] + src[k, pl.ds(base + 1, n, 2), :] for k in range(4)], axis=1)
            pairs = pairs.reshape(CHUNK // 2, 2, 16, Z)
            pairs = (pairs[:, 0] + pairs[:, 1]).reshape(CHUNK // 2 * 16, Z)
            put(dst, pl.ds(c * (CHUNK // 2 * 16), CHUNK // 2 * 16), times(pairs, half))
        return carry

    start = jnp.zeros((8, LANES), F32)
    part[pl.ds(0, 8), :], part[pl.ds(8, 8), :] = lax.fori_loop(0, X // CHUNK, load, (start, start))

    half = halving(256, 128)
    for src, dst in ((rm, rl), (cm, cl)):
        pairs = jnp.concatenate([src[k, pl.ds(0, 256, 2), :] + src[k, pl.ds(1, 256, 2), :] for k in range(2)], axis=1)
        pairs = pairs.reshape(16, 2, 8, 256)
        pairs = (pairs[:, 0] + pairs[:, 1]).reshape(128, 256)
        dst[...] = times(pairs, half)
    packed = 0.0
    for src, offset in ((rl, 0), (cl, 64)):
        quad = [sum(src[pl.ds(8 * f + 2 * j + e, 8, 16), :] for e in range(2) for f in range(2)) for j in range(4)]
        packed = packed + times(jnp.concatenate(quad, axis=0), halving(128, 128, offset))
    core[...] = packed
    sya[pl.ds(YB, 32), :] = packed
    syb[pl.ds(YB, 32), :] = packed

    inv = 0.8 / (0.09375 * 4.0 + cl[...])
    il[...] = inv
    gl[...] = inv * rl[...]
    for i in range(16):
        rows = pl.ds(8 * i, 8)
        c = gl[rows, :]
        total = in_plane(c, 0.0, 0.0)
        if i > 0:
            total = total + gl[pl.ds(8 * i - 8, 8), :]
        if i < 15:
            total = total + gl[pl.ds(8 * i + 8, 8), :]
        s2[rows, :] = il[rows, :] * (1.2 * rl[rows, :] + 0.0625 * total)

    def guess(i, carry):
        rows = pl.ds(64 * i, 64)
        inv = 0.8 / (1.5 + take(cm, rows))
        put(im, rows, inv)
        put(gm, pl.ds(64 * i + 16, 64), inv * take(rm, rows))
        return carry

    lax.fori_loop(0, 8, guess, 0)

    def layer(ref, rows, pad):
        return take(ref, pl.ds(rows * pad, rows))

    for hi in range(2):
        for base, g, inv, res, n, last, level in ((XF, g_s, i_s, r_v, Y, X - 1, 0), (XM, gm, im, rm, 16, 31, 1)):
            i = last * hi
            c, v = layer(g, n, i + 1), layer(inv, n, i)
            total = in_plane(c, 0.0, 0.0) + layer(g, n, i + (0 if hi else 2))
            lanes = g.shape[0]
            for a, value in enumerate((c, v, v * (1.2 * layer(res, n, i) + SCALE[level] * total))):
                for k in range(lanes):
                    fx[hi, pl.ds(base + (lanes * a + k) * n, n), :] = value[:, cols(k)]
        for a, ref in enumerate((gl, il, s2)):
            fx[hi, pl.ds(XL + a * 8, 8), :] = ref[pl.ds(hi * 15 * 8, 8), :]

    for a, (shift, pad) in enumerate(((0, 1), (0, 0), (1, 1))):
        for base, ref, n, width in ((YF, (g_s, i_s, g_s)[a], X, Y), (YM, (gm, im, gm)[a], 32, 16)):
            lanes = ref.shape[0]
            for k in range(lanes):
                late = lanes == 4 and a > 0
                start = (4 * (a - 1) + k) * n if late else base + (lanes * a + k) * n
                send(py, sza if late else sya, szb if late else syb, pl.ds(start, n),
                     ref[k, pl.ds(pad * width + shift, n, width), :],
                     ref[k, pl.ds(pad * width + width - 1 - shift, n, width), :])
        ref = (gl, il, gl)[a]
        send(py, sya, syb, pl.ds(YL + a * 16, 16), ref[pl.ds(shift, 16, 8), :], ref[pl.ds(7 - shift, 16, 8), :])


def smooth_kernel(r_v, g_s, i_s, rm, gm, im, s0, s1):
    def middle(i, carry):
        rows = pl.ds(16 * i, 16)
        c = take(gm, pl.ds(16 * i + 16, 16))
        total = in_plane(c, 0.0, 0.0) + (take(gm, rows) + take(gm, pl.ds(16 * i + 32, 16)))
        put(s1, rows, take(im, rows) * (1.2 * take(rm, rows) + 0.25 * total))
        return carry

    lax.fori_loop(0, 32, middle, 0, unroll=16)

    def fine(i, carry):
        rows = pl.ds(Y * i, Y)
        c = take(g_s, pl.ds(Y * i + Y, Y))
        total = in_plane(c, 0.0, 0.0) + (take(g_s, rows) + take(g_s, pl.ds(Y * i + 2 * Y, Y)))
        put(s0, rows, take(i_s, rows) * (1.2 * take(r_v, rows) + total))
        return carry

    lax.fori_loop(0, X, fine, 0, unroll=8)


def pick(slot, first, second, rows):
    return jnp.where(slot == 0, first[rows, :], second[rows, :])


class Halo:
    def __init__(self, **pairs):
        self.px, self.py, _ = parities()
        self.pairs = pairs

    def get(self, name, hi, start, n):
        parity = self.px if name == "rx" else self.py
        return pick(parity if hi else 1 - parity, *self.pairs[name], pl.ds(start, n))

    def layer(self, name, hi, start, n, lanes):
        return jnp.concatenate([self.get(name, hi, start + k * n, n) for k in range(lanes)], axis=1)

    def smoothed(self, along_y, hi, level, fx):
        lanes, n = 4 >> level, (X if along_y else Y) >> level
        if along_y:
            base = (YF, YM, YL)[level]
            if level == 0:
                g = self.layer("ry", hi, base, n, lanes)
                inv, beyond = [self.layer("rz", hi, a * lanes * n, n, lanes) for a in range(2)]
            else:
                g, inv, beyond = [self.layer("ry", hi, base + a * lanes * n, n, lanes) for a in range(3)]
            first, last = [self.layer("rx", xhi, XC + 7 * hi + (0, 4, 6)[level], 1, lanes) for xhi in range(2)]
            around = in_plane(g, first, last) + (beyond + self.layer("sy", hi, base, n, lanes))
            return 1.2 * g + SCALE[level] * inv * around, inv
        base = (XF, XM, XL)[level]
        inv, partly = [self.layer("rx", hi, base + a * lanes * n, n, lanes) for a in (1, 2)]
        own = jnp.concatenate([fx[hi, pl.ds(base + k * n, n), :] for k in range(lanes)], axis=1)
        return partly + SCALE[level] * inv * own, inv


def pack_kernel(fx, core, rya, ryb, r2a, r2b, block, outa, outb):
    _, _, qy = parities()
    halo = Halo(ry=(rya, ryb))
    block[pl.ds(0, 32), :] = pick(1 - qy, r2a, r2b, slice(None))
    block[pl.ds(32, 32), :] = halo.get("ry", 0, YB, 32)
    block[pl.ds(64, 32), :] = core[...]
    block[pl.ds(96, 32), :] = halo.get("ry", 1, YB, 32)
    block[pl.ds(128, 32), :] = pick(qy, r2a, r2b, slice(None))
    for out in (outa, outb):
        out[pl.ds(XB, 160), :] = block[...]
    sides = []
    for hi in range(2):
        rows, corner = [[], []], []
        for level, (base, ybase) in enumerate(((XF, YF), (XM, YM), (XL, YL))):
            lanes, n, long = 4 >> level, Y >> level, X >> level
            rows.append(fx[hi, pl.ds(base, 2 * lanes * n), :])
            edges = [[halo.get("ry", yhi, ybase + k * long + hi * (long - 1), 1) for yhi in range(2)] for k in range(lanes)]
            for k in range(lanes):
                inv = fx[hi, pl.ds(base + (lanes + k) * n, n), :]
                partly = fx[hi, pl.ds(base + (2 * lanes + k) * n, n), :]
                rows.append(partly + SCALE[level] * inv * ends(n, *edges[k]))
                for yhi in range(2):
                    rows[yhi].append(edges[k][yhi])
        corner = rows[0] + rows[1] + [jnp.zeros((2, LANES), F32)]
        sides.append((jnp.concatenate(rows[2:], axis=0), jnp.concatenate(corner, axis=0)))
    px = halo.px
    send(px, outa, outb, pl.ds(0, XB), sides[0][0], sides[1][0])
    send(px, outa, outb, pl.ds(XC, 16), sides[0][1], sides[1][1])


def ends(rows, first, last):
    row = iota((rows, LANES), 0)
    return jnp.where(row == 0, first, jnp.where(row == rows - 1, last, 0.0))


FACES = ((False, 0), (False, 1), (True, 0), (True, 1))
FACE_ROWS = (0, Y, 2 * Y, 2 * Y + X)


def coarse_kernel(s1, s2, fx, sya, syb, block, rya, ryb, rxa, rxb,
                  rep_m, fm, left_out,
                  bs, ga, gb, sz, low_s, rep_l, mid_s, fl):
    halo = Halo(sy=(sya, syb), rx=(rxa, rxb), ry=(rya, ryb))

    for n, value in enumerate((halo.get("rx", 0, XB, 160), block[...], halo.get("rx", 1, XB, 160))):
        bs[:, pl.ds(8 * n, 8), :] = value.reshape(20, 8, LANES)
    shape = (20, 24, LANES)
    live = iota(shape, 2) < 64
    both = bs[...]
    res = jnp.where(live, both, 0.0)
    coef = jnp.where(live, pltpu.roll(both, 64, 2), 0.0)
    inv = jnp.where(coef > 0.0, 0.8 / (0.09375 + coef), 0.0)
    zero = jnp.zeros((24, LANES), F32)
    for ref in (ga, gb):
        ref[0] = zero
        ref[21] = zero

    def around(ref):
        c = ref[pl.ds(1, 20)]
        total = ref[pl.ds(0, 20)] + ref[pl.ds(2, 20)]
        total = total + (pltpu.roll(c, 1, 1) + pltpu.roll(c, 23, 1))
        return c, total + (pltpu.roll(c, 1, 2) + pltpu.roll(c, LANES - 1, 2))

    ga[pl.ds(1, 20)] = inv * res
    bs[...] = inv
    now, new = ga, gb
    for _ in range(7):
        c, total = around(now)
        new[pl.ds(1, 20)] = c + bs[...] * (res - ((0.09375 + coef) * c - 0.015625 * total))
        now, new = new, now
    c, total = around(now)
    left = res - ((0.09375 + coef) * c - 0.015625 * total)
    leftover = jnp.sum(jnp.where(live[8:12, 8:16], left[8:12, 8:16], 0.0))
    sz[...] = times(now[pl.ds(8, 6)].reshape(144, LANES), doubling(LANES, LANES))

    left_out[...] = jnp.full((8, LANES), leftover, F32)

    for j in range(4):
        for e in range(2):
            for f in range(2):
                low_s[pl.ds(8 * f + 2 * j + e, 8, 16), :] = sz[pl.ds(24 * (j + 1) + 8, 8), :]
    low_s[...] = low_s[...] + s2[...]
    for hi in range(2):
        rows = pl.ds(hi * 120, 8)
        low_s[rows, :] = low_s[rows, :] + 0.0625 * fx[hi, pl.ds(XL + 8, 8), :] * halo.get("rx", hi, XL, 8)
    for hi in range(2):
        rows = pl.ds(hi * 7, 16, 8)
        low_s[rows, :] = low_s[rows, :] + 0.0625 * halo.get("sy", hi, YL + 16, 16) * halo.get("ry", hi, YL, 16)

    rep_l[pl.ds(0, 128, 2), :] = low_s[...]
    rep_l[pl.ds(1, 128, 2), :] = low_s[...]
    wide = times(rep_l[...], doubling(128, 256)).reshape(16, 1, 16, 256)
    wide = jnp.broadcast_to(wide, (16, 2, 16, 256)).reshape(512, 256)
    for k in range(2):
        mid_s[k] = wide[:, cols(k)] + s1[k]
    for hi in range(2):
        for k in range(2):
            rows = pl.ds(hi * 496, 16)
            mid_s[k, rows, :] = mid_s[k, rows, :] + (
                0.25 * fx[hi, pl.ds(XM + 32 + 16 * k, 16), :] * halo.get("rx", hi, XM + 16 * k, 16))
    for hi in range(2):
        for k in range(2):
            rows = pl.ds(hi * 15, 32, 16)
            mid_s[k, rows, :] = mid_s[k, rows, :] + (
                0.25 * halo.get("sy", hi, YM + 64 + 32 * k, 32) * halo.get("ry", hi, YM + 32 * k, 32))

    for k in range(2):
        rep_m[k, pl.ds(0, 512, 2), :] = mid_s[k]
        rep_m[k, pl.ds(1, 512, 2), :] = mid_s[k]
    for (along_y, hi), base in zip(FACES, FACE_ROWS):
        n = X if along_y else Y
        n2, n1 = n // 4, n // 2
        if along_y:
            top = sz[pl.ds(120 * hi + 8, 8), :]
        else:
            top = sz[pl.ds(24 + (16 if hi else 7), 4, 24), :]
        fl[pl.ds(0, n2 // 2, 2), :] = top
        fl[pl.ds(1, n2 // 2, 2), :] = top
        low = halo.smoothed(along_y, hi, 2, fx)[0] + fl[pl.ds(0, n2), :]
        fl[pl.ds(0, n2, 2), :] = low
        fl[pl.ds(1, n2, 2), :] = low
        wide = times(fl[pl.ds(0, n1), :], doubling(128, 256))
        middle = halo.smoothed(along_y, hi, 1, fx)[0] + wide
        for k in range(2):
            mid = middle[:, cols(k)]
            fm[k, pl.ds(base, n1, 2), :] = mid
            fm[k, pl.ds(base + 1, n1, 2), :] = mid


def fine_kernel(r_v, d_v, s0, rep_m, fm, left_in, part, fx, sya, syb, sza, szb, rya, ryb, rza, rzb, rxa, rxb,
                p, im, sums, hy):
    halo = Halo(sy=(sya, syb), sz=(sza, szb), rx=(rxa, rxb), ry=(rya, ryb), rz=(rza, rzb))
    twice = doubling(256, Z)

    def spread(i, carry):
        wide = times(take(rep_m, pl.ds(128 * i, 128)), twice).reshape(4, 1, Y, Z)
        wide = jnp.broadcast_to(wide, (4, 2, Y, Z)).reshape(8 * Y, Z)
        for k in range(4):
            p[k, pl.ds(8 * Y * i + Y, 8 * Y), :] = wide[:, cols(k)] + s0[k, pl.ds(8 * Y * i, 8 * Y), :]
        return carry

    lax.fori_loop(0, 8, spread, 0, unroll=2)
    for hi in range(2):
        for k in range(4):
            rows = pl.ds(Y + hi * (X - 1) * Y, Y)
            p[k, rows, :] = p[k, rows, :] + fx[hi, pl.ds(XF + (4 + k) * Y, Y), :] * halo.get("rx", hi, XF + k * Y, Y)
    for hi in range(2):
        for k in range(4):
            rows = pl.ds(Y + hi * (Y - 1), X, Y)
            p[k, rows, :] = p[k, rows, :] + halo.get("sz", hi, k * X, X) * halo.get("ry", hi, YF + k * X, X)

    outer = times(take(fm, pl.ds(0, 2 * (X + Y))), twice)
    for (along_y, hi), base in zip(FACES, FACE_ROWS):
        n = X if along_y else Y
        value, inv = halo.smoothed(along_y, hi, 0, fx)
        value = jnp.where(inv > 0.0, value + outer[base:base + n], 0.0)
        if along_y:
            hy[hi] = value
        else:
            put(p, pl.ds(hi * (X + 1) * Y, Y), value)

    def image(i, carry):
        rows = pl.ds(Y * i, Y)
        c = take(p, pl.ds(Y * i + Y, Y))
        around = in_plane(c, hy[0, pl.ds(i, 1), :], hy[1, pl.ds(i, 1), :])
        around = around + (take(p, rows) + take(p, pl.ds(Y * i + 2 * Y, Y)))
        dd, rr = take(d_v, rows), take(r_v, rows)
        out = (6.0 + dd) * c - around
        im[rows, :] = out
        return tuple(t + fold(v) for t, v in zip(carry, (rr * c, c * out, out)))

    start = jnp.zeros((8, LANES), F32)
    totals = lax.fori_loop(0, X, image, (start,) * 3, unroll=8)
    rz, zq, image_sum = [jnp.sum(t) for t in totals]
    totals = [rz, zq, jnp.sum(part[pl.ds(0, 8), :]), image_sum, jnp.sum(part[pl.ds(8, 8), :]), left_in[0:1, 0:1]]
    lane = iota((LANES, 8), 1)
    packed = jnp.zeros((LANES, 8), F32)
    for n, t in enumerate(totals):
        packed = jnp.where(lane == n, t, packed)
    sums[...] = packed


def final_kernel(every, r_v, d_v, p, im, update, residual):
    step = pl.program_id(0)
    gx, gy = lax.axis_index("gx"), lax.axis_index("gy")
    total = jnp.sum(every[...], axis=0, keepdims=True)
    lane8 = iota((1, 8), 1)
    rz, zq, res_sum, image_sum, coef_sum, left = [jnp.sum(jnp.where(lane8 == n, total, 0.0), axis=1, keepdims=True) for n in range(6)]
    shift = left / (coef_sum / 512.0 + 6.0 * 64.0 * 64.0 / 64.0)
    ones_sum = coef_sum + 6.0 * WHOLE * WHOLE
    alpha = (rz + shift * res_sum) / (zq + shift * (2.0 * image_sum + shift * ones_sum))
    scaled = alpha * shift
    row, lane = iota((Y, Z), 0), iota((Y, Z), 1)
    walls = jnp.where(lane == 0, 1.0, 0.0) + jnp.where(lane == Z - 1, 1.0, 0.0)
    walls = walls + jnp.where((row == 0) & (gy == 0), 1.0, 0.0)
    walls = walls + jnp.where((row == Y - 1) & (gy == DEVS_Y - 1), 1.0, 0.0)

    def plane(i, carry):
        x = step * CHUNK + i
        end = ((x == 0) & (gx == 0)) | ((x == X - 1) & (gx == DEVS_X - 1))
        rows = pl.ds(x * Y, Y)
        outside = walls + jnp.where(end, 1.0, 0.0)
        here = pl.ds(i * Y, Y)
        update[here, :] = alpha * take(p, pl.ds(x * Y + Y, Y)) + scaled
        residual[here, :] = take(r_v, rows) - alpha * im[rows, :] - scaled * (take(d_v, rows) + outside)
        return carry

    lax.fori_loop(0, CHUNK, plane, 0, unroll=2)


def f32(*shape):
    return jax.ShapeDtypeStruct(shape, F32)


def resident(*shape):
    return pltpu.VMEM(shape, F32)


def in_vmem(value):
    return pltpu.with_memory_space_constraint(value, pltpu.VMEM)


VM = pl.BlockSpec(memory_space=pltpu.VMEM)


def swap(value, axis, distance, offset):
    count = lax.axis_size(axis)
    pairs = []
    for i in range(count - distance):
        if (i // distance) % 2 == offset:
            pairs += [(i, i + distance), (i + distance, i)]
    return lax.ppermute(value, axis, pairs)


def body(right_side, diagonal):
    r = right_side.reshape(X * Y, Z)
    d = diagonal.reshape(X * Y, Z)
    vm = pltpu.VMEM
    hbm = pl.BlockSpec(memory_space=pl.ANY)
    r_v, d_v, g, inv, fx, sya, syb, sza, szb, core, rm, gm, im1, s2, part = pl.pallas_call(
        restrict_kernel,
        in_specs=[hbm, hbm],
        out_specs=[VM] * 15,
        out_shape=[resident(4, X * Y, LANES)] * 2 + [resident(4, (X + 2) * Y, LANES), resident(4, X * Y, LANES)]
        + [resident(2, XB, LANES)] + [resident(YROWS, LANES)] * 2 + [resident(ZROWS, LANES)] * 2 + [resident(32, LANES), resident(2, 512, LANES)]
        + [resident(2, 544, LANES), resident(2, 512, LANES), resident(128, 128), resident(16, LANES)],
        scratch_shapes=[vm((2, 512, LANES), F32)] + [vm((128, 128), F32)] * 4
        + [pltpu.SemaphoreType.DMA((2, X // CHUNK, 4))],
        compiler_params=pltpu.CompilerParams(vmem_limit_bytes=12 * 2**20),
        name="restrict_all",
    )(pltpu.with_memory_space_constraint(r, pltpu.HBM), pltpu.with_memory_space_constraint(d, pltpu.HBM))

    rya = swap(sya, "gy", 1, 0)
    ryb = swap(syb, "gy", 1, 1)
    r2a = swap(core, "gy", 2, 0)
    r2b = swap(core, "gy", 2, 1)
    s0, s1 = pl.pallas_call(
        smooth_kernel,
        in_specs=[VM] * 6,
        out_specs=[VM] * 2,
        out_shape=[resident(4, X * Y, LANES), resident(2, 512, LANES)],
        compiler_params=pltpu.CompilerParams(vmem_limit_bytes=4 * 2**20),
        cost_estimate=pl.CostEstimate(flops=COST, transcendentals=0, bytes_accessed=0),
        name="smooth_own",
    )(in_vmem(r_v), in_vmem(g), in_vmem(inv), in_vmem(rm), in_vmem(gm), in_vmem(im1))
    block, outa, outb = pl.pallas_call(
        pack_kernel,
        in_specs=[VM] * 6,
        out_specs=[VM] * 3,
        out_shape=[resident(160, LANES)] + [resident(XROWS, LANES)] * 2,
        compiler_params=pltpu.CompilerParams(vmem_limit_bytes=2 * 2**20),
        name="pack_faces",
    )(in_vmem(fx), in_vmem(core), rya, ryb, r2a, r2b)
    rxa = swap(outa, "gx", 1, 0)
    rxb = swap(outb, "gx", 1, 1)
    rza = swap(sza, "gy", 1, 0)
    rzb = swap(szb, "gy", 1, 1)

    rep, faces, left = pl.pallas_call(
        coarse_kernel,
        in_specs=[VM] * 10,
        out_specs=[VM] * 3,
        out_shape=[resident(2, 1024, LANES), resident(2, 2 * (X + Y), LANES), resident(8, LANES)],
        scratch_shapes=[vm((20, 24, LANES), F32), vm((22, 24, LANES), F32), vm((22, 24, LANES), F32), vm((144, LANES), F32),
                        vm((128, 128), F32), vm((256, 128), F32), vm((2, 512, LANES), F32), vm((32, LANES), F32)],
        compiler_params=pltpu.CompilerParams(vmem_limit_bytes=8 * 2**20),
        cost_estimate=pl.CostEstimate(flops=COST, transcendentals=0, bytes_accessed=0),
        name="solve_coarse",
    )(in_vmem(s1), in_vmem(s2), in_vmem(fx), in_vmem(sya), in_vmem(syb), in_vmem(block), rya, ryb, rxa, rxb)
    p, im, sums = pl.pallas_call(
        fine_kernel,
        in_specs=[VM] * 18,
        out_specs=[VM] * 3,
        out_shape=[resident(4, (X + 2) * Y, LANES), resident(X * Y, Z), f32(LANES, 8)],
        scratch_shapes=[vm((2, X, Z), F32)],
        compiler_params=pltpu.CompilerParams(vmem_limit_bytes=8 * 2**20),
        name="solve_fine",
    )(in_vmem(r_v), in_vmem(d_v), in_vmem(s0), in_vmem(rep), in_vmem(faces), in_vmem(left),
      in_vmem(part), in_vmem(fx), in_vmem(sya), in_vmem(syb), in_vmem(sza), in_vmem(szb), rya, ryb, rza, rzb, rxa, rxb)

    every = lax.all_to_all(sums, ("gx", "gy"), 0, 0, tiled=True)
    blocks = pl.BlockSpec((CHUNK * Y, Z), lambda i: (i, 0))
    update, residual = pl.pallas_call(
        final_kernel,
        grid=(X // CHUNK,),
        in_specs=[VM] * 5,
        out_specs=[blocks, blocks],
        out_shape=[f32(X * Y, Z), f32(X * Y, Z)],
        compiler_params=pltpu.CompilerParams(vmem_limit_bytes=8 * 2**20),
        name="scale_outputs",
    )(every, in_vmem(r_v), in_vmem(d_v), in_vmem(p), in_vmem(im))
    return update.reshape(X, Y, Z), residual.reshape(X, Y, Z)


def solution(mesh):
    return jax.shard_map(
        body,
        mesh=mesh,
        in_specs=(P("gx", "gy", None), P("gx", "gy", None)),
        out_specs=(P("gx", "gy", None), P("gx", "gy", None)),
        check_vma=False,
    )
```

```python
import jax
import jax.numpy as jnp
from jax import lax
from jax.experimental import pallas as pl
from jax.experimental.pallas import tpu as pltpu
from jax.sharding import PartitionSpec as P


F32 = jnp.float32
BF16 = jnp.bfloat16

X, Y, Z = 64, 32, 512
DEVS_X, DEVS_Y = 8, 16
WHOLE = 512
LANES = 128
COST = 20_000_000
CHUNK = 16
OUT = 16

XF, XM, XL, XB, XC, XROWS = 0, 384, 480, 504, 664, 680
YF, YM, YL, YB, YROWS = 0, 256, 448, 496, 528
ZROWS = 512
SCALE = (1.0, 0.25, 0.0625)


def iota(shape, axis):
    return lax.broadcasted_iota(jnp.int32, shape, axis)


def halving(depth, cols, offset=0):
    coarse = lax.shift_right_logical(iota((depth, cols), 0), 1) + offset
    return jnp.where(coarse == iota((depth, cols), 1), 0.125, 0.0).astype(BF16)


def doubling(depth, cols):
    coarse = lax.shift_right_logical(iota((depth, cols), 1), 1)
    return jnp.where(coarse == iota((depth, cols), 0), 1.0, 0.0).astype(BF16)


def times(value, table):
    high = value.astype(BF16)
    low = (value - high.astype(F32)).astype(BF16)
    return jnp.dot(high, table, preferred_element_type=F32) + jnp.dot(low, table, preferred_element_type=F32)


def in_plane(c, top, bottom):
    rows, lanes = c.shape
    row, lane = iota(c.shape, 0), iota(c.shape, 1)
    up = jnp.where(row == 0, top, pltpu.roll(c, 1, 0))
    down = jnp.where(row == rows - 1, bottom, pltpu.roll(c, rows - 1, 0))
    left = jnp.where(lane == 0, 0.0, pltpu.roll(c, 1, 1))
    right = jnp.where(lane == lanes - 1, 0.0, pltpu.roll(c, lanes - 1, 1))
    return (up + down) + (left + right)


def cols(k):
    return slice(LANES * k, LANES * (k + 1))


def take(ref, rows):
    return jnp.concatenate([ref[k, rows, :] for k in range(ref.shape[0])], axis=1)


def put(ref, rows, value):
    for k in range(ref.shape[0]):
        ref[k, rows, :] = value[:, cols(k)]


def fold(v):
    v = (v[0:8] + v[8:16]) + (v[16:24] + v[24:32])
    return (v[:, cols(0)] + v[:, cols(1)]) + (v[:, cols(2)] + v[:, cols(3)])


def send(up, down, rows, low, high):
    up[rows, :] = high
    down[rows, :] = low


def beside(value, hi, axis, distance=1):
    index = lax.axis_index(axis)
    outside = index + distance >= lax.axis_size(axis) if hi else index < distance
    return jnp.where(outside, 0.0, value)


def restrict_kernel(r_hbm, d_hbm, r_v, d_v, g_s, i_s, fx, sya, syb, sza, szb, core, rm, gm, im, s2, part,
                    cm, rl, cl, gl, il, sems):
    def copies(c):
        rows = pl.ds(c * CHUNK * Y, CHUNK * Y)
        for n, (src, dst) in enumerate(((r_hbm, r_v), (d_hbm, d_v))):
            for k in range(4):
                yield pltpu.make_async_copy(src.at[rows, pl.ds(LANES * k, LANES)], dst.at[k, rows], sems.at[n, c, k])

    for c in range(X // CHUNK):
        for one in copies(c):
            one.start()

    for k in range(4):
        g_s[k, pl.ds(0, Y), :] = jnp.zeros((Y, LANES), F32)
        g_s[k, pl.ds((X + 1) * Y, Y), :] = jnp.zeros((Y, LANES), F32)
    for k in range(2):
        gm[k, pl.ds(0, 16), :] = jnp.zeros((16, LANES), F32)
        gm[k, pl.ds(33 * 16, 16), :] = jnp.zeros((16, LANES), F32)
    half = halving(512, 256)

    def load(c, carry):
        for one in copies(c):
            one.wait()
        base = c * CHUNK * Y

        def plane(i, carry):
            rows = pl.ds(base + i * Y, Y)
            dd, rr = take(d_v, rows), take(r_v, rows)
            inv = 0.8 / (6.0 + dd)
            put(i_s, rows, inv)
            put(g_s, pl.ds(base + (i + 1) * Y, Y), inv * rr)
            return carry[0] + fold(rr), carry[1] + fold(dd)

        carry = lax.fori_loop(0, CHUNK, plane, carry, unroll=4)
        n = CHUNK * Y // 2
        for src, dst in ((r_v, rm), (d_v, cm)):
            pairs = jnp.concatenate(
                [src[k, pl.ds(base, n, 2), :] + src[k, pl.ds(base + 1, n, 2), :] for k in range(4)], axis=1)
            pairs = pairs.reshape(CHUNK // 2, 2, 16, Z)
            pairs = (pairs[:, 0] + pairs[:, 1]).reshape(CHUNK // 2 * 16, Z)
            put(dst, pl.ds(c * (CHUNK // 2 * 16), CHUNK // 2 * 16), times(pairs, half))
        return carry

    start = jnp.zeros((8, LANES), F32)
    part[pl.ds(0, 8), :], part[pl.ds(8, 8), :] = lax.fori_loop(0, X // CHUNK, load, (start, start))

    half = halving(256, 128)
    for src, dst in ((rm, rl), (cm, cl)):
        pairs = jnp.concatenate([src[k, pl.ds(0, 256, 2), :] + src[k, pl.ds(1, 256, 2), :] for k in range(2)], axis=1)
        pairs = pairs.reshape(16, 2, 8, 256)
        pairs = (pairs[:, 0] + pairs[:, 1]).reshape(128, 256)
        dst[...] = times(pairs, half)
    packed = 0.0
    for src, offset in ((rl, 0), (cl, 64)):
        quad = [sum(src[pl.ds(8 * f + 2 * j + e, 8, 16), :] for e in range(2) for f in range(2)) for j in range(4)]
        packed = packed + times(jnp.concatenate(quad, axis=0), halving(128, 128, offset))
    core[...] = packed
    sya[pl.ds(YB, 32), :] = packed
    syb[pl.ds(YB, 32), :] = packed

    inv = 0.8 / (0.09375 * 4.0 + cl[...])
    il[...] = inv
    gl[...] = inv * rl[...]
    for i in range(16):
        rows = pl.ds(8 * i, 8)
        c = gl[rows, :]
        total = in_plane(c, 0.0, 0.0)
        if i > 0:
            total = total + gl[pl.ds(8 * i - 8, 8), :]
        if i < 15:
            total = total + gl[pl.ds(8 * i + 8, 8), :]
        s2[rows, :] = il[rows, :] * (1.2 * rl[rows, :] + 0.0625 * total)

    def guess(i, carry):
        rows = pl.ds(64 * i, 64)
        inv = 0.8 / (1.5 + take(cm, rows))
        put(im, rows, inv)
        put(gm, pl.ds(64 * i + 16, 64), inv * take(rm, rows))
        return carry

    lax.fori_loop(0, 8, guess, 0)

    def layer(ref, rows, pad):
        return take(ref, pl.ds(rows * pad, rows))

    for hi in range(2):
        for base, g, inv, res, n, last, level in ((XF, g_s, i_s, r_v, Y, X - 1, 0), (XM, gm, im, rm, 16, 31, 1)):
            i = last * hi
            c, v = layer(g, n, i + 1), layer(inv, n, i)
            total = in_plane(c, 0.0, 0.0) + layer(g, n, i + (0 if hi else 2))
            lanes = g.shape[0]
            for a, value in enumerate((c, v, v * (1.2 * layer(res, n, i) + SCALE[level] * total))):
                for k in range(lanes):
                    fx[hi, pl.ds(base + (lanes * a + k) * n, n), :] = value[:, cols(k)]
        for a, ref in enumerate((gl, il, s2)):
            fx[hi, pl.ds(XL + a * 8, 8), :] = ref[pl.ds(hi * 15 * 8, 8), :]

    for a, (shift, pad) in enumerate(((0, 1), (0, 0), (1, 1))):
        for base, ref, n, width in ((YF, (g_s, i_s, g_s)[a], X, Y), (YM, (gm, im, gm)[a], 32, 16)):
            lanes = ref.shape[0]
            for k in range(lanes):
                late = lanes == 4 and a > 0
                start = (4 * (a - 1) + k) * n if late else base + (lanes * a + k) * n
                send(sza if late else sya, szb if late else syb, pl.ds(start, n),
                     ref[k, pl.ds(pad * width + shift, n, width), :],
                     ref[k, pl.ds(pad * width + width - 1 - shift, n, width), :])
        ref = (gl, il, gl)[a]
        send(sya, syb, pl.ds(YL + a * 16, 16), ref[pl.ds(shift, 16, 8), :], ref[pl.ds(7 - shift, 16, 8), :])


def smooth_kernel(r_v, g_s, i_s, rm, gm, im, s0, s1):
    def middle(i, carry):
        rows = pl.ds(16 * i, 16)
        c = take(gm, pl.ds(16 * i + 16, 16))
        total = in_plane(c, 0.0, 0.0) + (take(gm, rows) + take(gm, pl.ds(16 * i + 32, 16)))
        put(s1, rows, take(im, rows) * (1.2 * take(rm, rows) + 0.25 * total))
        return carry

    lax.fori_loop(0, 32, middle, 0, unroll=16)

    def fine(i, carry):
        rows = pl.ds(Y * i, Y)
        c = take(g_s, pl.ds(Y * i + Y, Y))
        total = in_plane(c, 0.0, 0.0) + (take(g_s, rows) + take(g_s, pl.ds(Y * i + 2 * Y, Y)))
        put(s0, rows, take(i_s, rows) * (1.2 * take(r_v, rows) + total))
        return carry

    lax.fori_loop(0, X, fine, 0, unroll=8)


class Halo:
    def __init__(self, **pairs):
        self.pairs = pairs

    def get(self, name, hi, start, n):
        value = self.pairs[name][1 - hi][pl.ds(start, n), :]
        if name[0] == "s":
            return value
        return beside(value, hi, "gx" if name == "rx" else "gy")

    def layer(self, name, hi, start, n, lanes):
        return jnp.concatenate([self.get(name, hi, start + k * n, n) for k in range(lanes)], axis=1)

    def smoothed(self, along_y, hi, level, fx):
        lanes, n = 4 >> level, (X if along_y else Y) >> level
        if along_y:
            base = (YF, YM, YL)[level]
            if level == 0:
                g = self.layer("ry", hi, base, n, lanes)
                inv, beyond = [self.layer("rz", hi, a * lanes * n, n, lanes) for a in range(2)]
            else:
                g, inv, beyond = [self.layer("ry", hi, base + a * lanes * n, n, lanes) for a in range(3)]
            first, last = [self.layer("rx", xhi, XC + 7 * hi + (0, 4, 6)[level], 1, lanes) for xhi in range(2)]
            around = in_plane(g, first, last) + (beyond + self.layer("sy", hi, base, n, lanes))
            return 1.2 * g + SCALE[level] * inv * around, inv
        base = (XF, XM, XL)[level]
        inv, partly = [self.layer("rx", hi, base + a * lanes * n, n, lanes) for a in (1, 2)]
        own = jnp.concatenate([fx[hi, pl.ds(base + k * n, n), :] for k in range(lanes)], axis=1)
        return partly + SCALE[level] * inv * own, inv


def pack_kernel(fx, core, rya, ryb, r2a, r2b, block, outa, outb):
    halo = Halo(ry=(rya, ryb))
    block[pl.ds(0, 32), :] = beside(r2b[...], 0, "gy", 2)
    block[pl.ds(32, 32), :] = halo.get("ry", 0, YB, 32)
    block[pl.ds(64, 32), :] = core[...]
    block[pl.ds(96, 32), :] = halo.get("ry", 1, YB, 32)
    block[pl.ds(128, 32), :] = beside(r2a[...], 1, "gy", 2)
    for out in (outa, outb):
        out[pl.ds(XB, 160), :] = block[...]
    sides = []
    for hi in range(2):
        rows, corner = [[], []], []
        for level, (base, ybase) in enumerate(((XF, YF), (XM, YM), (XL, YL))):
            lanes, n, long = 4 >> level, Y >> level, X >> level
            rows.append(fx[hi, pl.ds(base, 2 * lanes * n), :])
            edges = [[halo.get("ry", yhi, ybase + k * long + hi * (long - 1), 1) for yhi in range(2)] for k in range(lanes)]
            for k in range(lanes):
                inv = fx[hi, pl.ds(base + (lanes + k) * n, n), :]
                partly = fx[hi, pl.ds(base + (2 * lanes + k) * n, n), :]
                rows.append(partly + SCALE[level] * inv * ends(n, *edges[k]))
                for yhi in range(2):
                    rows[yhi].append(edges[k][yhi])
        corner = rows[0] + rows[1] + [jnp.zeros((2, LANES), F32)]
        sides.append((jnp.concatenate(rows[2:], axis=0), jnp.concatenate(corner, axis=0)))
    send(outa, outb, pl.ds(0, XB), sides[0][0], sides[1][0])
    send(outa, outb, pl.ds(XC, 16), sides[0][1], sides[1][1])


def ends(rows, first, last):
    row = iota((rows, LANES), 0)
    return jnp.where(row == 0, first, jnp.where(row == rows - 1, last, 0.0))


FACES = ((False, 0), (False, 1), (True, 0), (True, 1))
FACE_ROWS = (0, Y, 2 * Y, 2 * Y + X)


def coarse_kernel(s1, s2, fx, sya, syb, block, rya, ryb, rxa, rxb,
                  rep_m, fm, left_out,
                  bs, ga, gb, sz, low_s, rep_l, mid_s, fl):
    halo = Halo(sy=(sya, syb), rx=(rxa, rxb), ry=(rya, ryb))

    for n, value in enumerate((halo.get("rx", 0, XB, 160), block[...], halo.get("rx", 1, XB, 160))):
        bs[:, pl.ds(8 * n, 8), :] = value.reshape(20, 8, LANES)
    shape = (20, 24, LANES)
    live = iota(shape, 2) < 64
    both = bs[...]
    res = jnp.where(live, both, 0.0)
    coef = jnp.where(live, pltpu.roll(both, 64, 2), 0.0)
    inv = jnp.where(coef > 0.0, 0.8 / (0.09375 + coef), 0.0)
    zero = jnp.zeros((24, LANES), F32)
    for ref in (ga, gb):
        ref[0] = zero
        ref[21] = zero

    def around(ref):
        c = ref[pl.ds(1, 20)]
        total = ref[pl.ds(0, 20)] + ref[pl.ds(2, 20)]
        total = total + (pltpu.roll(c, 1, 1) + pltpu.roll(c, 23, 1))
        return c, total + (pltpu.roll(c, 1, 2) + pltpu.roll(c, LANES - 1, 2))

    ga[pl.ds(1, 20)] = inv * res
    bs[...] = inv
    now, new = ga, gb
    for _ in range(7):
        c, total = around(now)
        new[pl.ds(1, 20)] = c + bs[...] * (res - ((0.09375 + coef) * c - 0.015625 * total))
        now, new = new, now
    c, total = around(now)
    left = res - ((0.09375 + coef) * c - 0.015625 * total)
    leftover = jnp.sum(jnp.where(live[8:12, 8:16], left[8:12, 8:16], 0.0))
    sz[...] = times(now[pl.ds(8, 6)].reshape(144, LANES), doubling(LANES, LANES))

    left_out[...] = jnp.full((8, LANES), leftover, F32)

    for j in range(4):
        for e in range(2):
            for f in range(2):
                low_s[pl.ds(8 * f + 2 * j + e, 8, 16), :] = sz[pl.ds(24 * (j + 1) + 8, 8), :]
    low_s[...] = low_s[...] + s2[...]
    for hi in range(2):
        rows = pl.ds(hi * 120, 8)
        low_s[rows, :] = low_s[rows, :] + 0.0625 * fx[hi, pl.ds(XL + 8, 8), :] * halo.get("rx", hi, XL, 8)
    for hi in range(2):
        rows = pl.ds(hi * 7, 16, 8)
        low_s[rows, :] = low_s[rows, :] + 0.0625 * halo.get("sy", hi, YL + 16, 16) * halo.get("ry", hi, YL, 16)

    rep_l[pl.ds(0, 128, 2), :] = low_s[...]
    rep_l[pl.ds(1, 128, 2), :] = low_s[...]
    wide = times(rep_l[...], doubling(128, 256)).reshape(16, 1, 16, 256)
    wide = jnp.broadcast_to(wide, (16, 2, 16, 256)).reshape(512, 256)
    for k in range(2):
        mid_s[k] = wide[:, cols(k)] + s1[k]
    for hi in range(2):
        for k in range(2):
            rows = pl.ds(hi * 496, 16)
            mid_s[k, rows, :] = mid_s[k, rows, :] + (
                0.25 * fx[hi, pl.ds(XM + 32 + 16 * k, 16), :] * halo.get("rx", hi, XM + 16 * k, 16))
    for hi in range(2):
        for k in range(2):
            rows = pl.ds(hi * 15, 32, 16)
            mid_s[k, rows, :] = mid_s[k, rows, :] + (
                0.25 * halo.get("sy", hi, YM + 64 + 32 * k, 32) * halo.get("ry", hi, YM + 32 * k, 32))

    for k in range(2):
        rep_m[k, pl.ds(0, 512, 2), :] = mid_s[k]
        rep_m[k, pl.ds(1, 512, 2), :] = mid_s[k]
    for (along_y, hi), base in zip(FACES, FACE_ROWS):
        n = X if along_y else Y
        n2, n1 = n // 4, n // 2
        if along_y:
            top = sz[pl.ds(120 * hi + 8, 8), :]
        else:
            top = sz[pl.ds(24 + (16 if hi else 7), 4, 24), :]
        fl[pl.ds(0, n2 // 2, 2), :] = top
        fl[pl.ds(1, n2 // 2, 2), :] = top
        low = halo.smoothed(along_y, hi, 2, fx)[0] + fl[pl.ds(0, n2), :]
        fl[pl.ds(0, n2, 2), :] = low
        fl[pl.ds(1, n2, 2), :] = low
        wide = times(fl[pl.ds(0, n1), :], doubling(128, 256))
        middle = halo.smoothed(along_y, hi, 1, fx)[0] + wide
        for k in range(2):
            mid = middle[:, cols(k)]
            fm[k, pl.ds(base, n1, 2), :] = mid
            fm[k, pl.ds(base + 1, n1, 2), :] = mid


def fine_kernel(r_v, d_v, s0, rep_m, fm, left_in, part, fx, sya, syb, sza, szb, rya, ryb, rza, rzb, rxa, rxb,
                p, im, sums, hy):
    halo = Halo(sy=(sya, syb), sz=(sza, szb), rx=(rxa, rxb), ry=(rya, ryb), rz=(rza, rzb))
    twice = doubling(256, Z)

    def spread(i, carry):
        wide = times(take(rep_m, pl.ds(128 * i, 128)), twice).reshape(4, 1, Y, Z)
        wide = jnp.broadcast_to(wide, (4, 2, Y, Z)).reshape(8 * Y, Z)
        for k in range(4):
            p[k, pl.ds(8 * Y * i + Y, 8 * Y), :] = wide[:, cols(k)] + s0[k, pl.ds(8 * Y * i, 8 * Y), :]
        return carry

    lax.fori_loop(0, 8, spread, 0, unroll=2)
    for hi in range(2):
        for k in range(4):
            rows = pl.ds(Y + hi * (X - 1) * Y, Y)
            p[k, rows, :] = p[k, rows, :] + fx[hi, pl.ds(XF + (4 + k) * Y, Y), :] * halo.get("rx", hi, XF + k * Y, Y)
    for hi in range(2):
        for k in range(4):
            rows = pl.ds(Y + hi * (Y - 1), X, Y)
            p[k, rows, :] = p[k, rows, :] + halo.get("sz", hi, k * X, X) * halo.get("ry", hi, YF + k * X, X)

    outer = times(take(fm, pl.ds(0, 2 * (X + Y))), twice)
    for (along_y, hi), base in zip(FACES, FACE_ROWS):
        n = X if along_y else Y
        value, inv = halo.smoothed(along_y, hi, 0, fx)
        value = jnp.where(inv > 0.0, value + outer[base:base + n], 0.0)
        if along_y:
            hy[hi] = value
        else:
            put(p, pl.ds(hi * (X + 1) * Y, Y), value)

    def image(i, carry):
        rows = pl.ds(Y * i, Y)
        c = take(p, pl.ds(Y * i + Y, Y))
        around = in_plane(c, hy[0, pl.ds(i, 1), :], hy[1, pl.ds(i, 1), :])
        around = around + (take(p, rows) + take(p, pl.ds(Y * i + 2 * Y, Y)))
        dd, rr = take(d_v, rows), take(r_v, rows)
        out = (6.0 + dd) * c - around
        im[rows, :] = out
        return tuple(t + fold(v) for t, v in zip(carry, (rr * c, c * out, out)))

    start = jnp.zeros((8, LANES), F32)
    totals = lax.fori_loop(0, X, image, (start,) * 3, unroll=8)
    rz, zq, image_sum = [jnp.sum(t) for t in totals]
    totals = [rz, zq, jnp.sum(part[pl.ds(0, 8), :]), image_sum, jnp.sum(part[pl.ds(8, 8), :]), left_in[0:1, 0:1]]
    lane = iota((LANES, 8), 1)
    packed = jnp.zeros((LANES, 8), F32)
    for n, t in enumerate(totals):
        packed = jnp.where(lane == n, t, packed)
    sums[...] = packed


def final_kernel(every, r_v, d_v, p, im, update, residual):
    step = pl.program_id(0)
    gx, gy = lax.axis_index("gx"), lax.axis_index("gy")
    total = jnp.sum(every[...], axis=0, keepdims=True)
    lane8 = iota((1, 8), 1)
    rz, zq, res_sum, image_sum, coef_sum, left = [jnp.sum(jnp.where(lane8 == n, total, 0.0), axis=1, keepdims=True) for n in range(6)]
    shift = left / (coef_sum / 512.0 + 6.0 * 64.0 * 64.0 / 64.0)
    ones_sum = coef_sum + 6.0 * WHOLE * WHOLE
    alpha = (rz + shift * res_sum) / (zq + shift * (2.0 * image_sum + shift * ones_sum))
    scaled = alpha * shift
    row, lane = iota((Y, Z), 0), iota((Y, Z), 1)
    walls = jnp.where(lane == 0, 1.0, 0.0) + jnp.where(lane == Z - 1, 1.0, 0.0)
    walls = walls + jnp.where((row == 0) & (gy == 0), 1.0, 0.0)
    walls = walls + jnp.where((row == Y - 1) & (gy == DEVS_Y - 1), 1.0, 0.0)

    def plane(i, carry):
        x = step * OUT + i
        end = ((x == 0) & (gx == 0)) | ((x == X - 1) & (gx == DEVS_X - 1))
        rows = pl.ds(x * Y, Y)
        outside = walls + jnp.where(end, 1.0, 0.0)
        here = pl.ds(i * Y, Y)
        update[here, :] = alpha * take(p, pl.ds(x * Y + Y, Y)) + scaled
        residual[here, :] = take(r_v, rows) - alpha * im[rows, :] - scaled * (take(d_v, rows) + outside)
        return carry

    lax.fori_loop(0, OUT, plane, 0, unroll=8)


def f32(*shape):
    return jax.ShapeDtypeStruct(shape, F32)


def resident(*shape):
    return pltpu.VMEM(shape, F32)


def in_vmem(value):
    return pltpu.with_memory_space_constraint(value, pltpu.VMEM)


VM = pl.BlockSpec(memory_space=pltpu.VMEM)


def shift(value, axis, distance):
    count = lax.axis_size(axis)
    return lax.ppermute(value, axis, [(i, (i + distance) % count) for i in range(count)])


def body(right_side, diagonal):
    r = right_side.reshape(X * Y, Z)
    d = diagonal.reshape(X * Y, Z)
    vm = pltpu.VMEM
    hbm = pl.BlockSpec(memory_space=pl.ANY)
    r_v, d_v, g, inv, fx, sya, syb, sza, szb, core, rm, gm, im1, s2, part = pl.pallas_call(
        restrict_kernel,
        in_specs=[hbm, hbm],
        out_specs=[VM] * 15,
        out_shape=[resident(4, X * Y, LANES)] * 2 + [resident(4, (X + 2) * Y, LANES), resident(4, X * Y, LANES)]
        + [resident(2, XB, LANES)] + [resident(YROWS, LANES)] * 2 + [resident(ZROWS, LANES)] * 2 + [resident(32, LANES), resident(2, 512, LANES)]
        + [resident(2, 544, LANES), resident(2, 512, LANES), resident(128, 128), resident(16, LANES)],
        scratch_shapes=[vm((2, 512, LANES), F32)] + [vm((128, 128), F32)] * 4
        + [pltpu.SemaphoreType.DMA((2, X // CHUNK, 4))],
        compiler_params=pltpu.CompilerParams(vmem_limit_bytes=12 * 2**20),
        name="restrict_all",
    )(pltpu.with_memory_space_constraint(r, pltpu.HBM), pltpu.with_memory_space_constraint(d, pltpu.HBM))

    rya = shift(syb, "gy", -1)
    ryb = shift(sya, "gy", 1)
    r2a = shift(core, "gy", -2)
    r2b = shift(core, "gy", 2)
    s0, s1 = pl.pallas_call(
        smooth_kernel,
        in_specs=[VM] * 6,
        out_specs=[VM] * 2,
        out_shape=[resident(4, X * Y, LANES), resident(2, 512, LANES)],
        compiler_params=pltpu.CompilerParams(vmem_limit_bytes=4 * 2**20),
        cost_estimate=pl.CostEstimate(flops=COST, transcendentals=0, bytes_accessed=0),
        name="smooth_own",
    )(in_vmem(r_v), in_vmem(g), in_vmem(inv), in_vmem(rm), in_vmem(gm), in_vmem(im1))
    block, outa, outb = pl.pallas_call(
        pack_kernel,
        in_specs=[VM] * 6,
        out_specs=[VM] * 3,
        out_shape=[resident(160, LANES)] + [resident(XROWS, LANES)] * 2,
        compiler_params=pltpu.CompilerParams(vmem_limit_bytes=2 * 2**20),
        name="pack_faces",
    )(in_vmem(fx), in_vmem(core), rya, ryb, r2a, r2b)
    rxa = shift(outb, "gx", -1)
    rxb = shift(outa, "gx", 1)
    rza = shift(szb, "gy", -1)
    rzb = shift(sza, "gy", 1)

    rep, faces, left = pl.pallas_call(
        coarse_kernel,
        in_specs=[VM] * 10,
        out_specs=[VM] * 3,
        out_shape=[resident(2, 1024, LANES), resident(2, 2 * (X + Y), LANES), resident(8, LANES)],
        scratch_shapes=[vm((20, 24, LANES), F32), vm((22, 24, LANES), F32), vm((22, 24, LANES), F32), vm((144, LANES), F32),
                        vm((128, 128), F32), vm((256, 128), F32), vm((2, 512, LANES), F32), vm((32, LANES), F32)],
        compiler_params=pltpu.CompilerParams(vmem_limit_bytes=8 * 2**20),
        cost_estimate=pl.CostEstimate(flops=COST, transcendentals=0, bytes_accessed=0),
        name="solve_coarse",
    )(in_vmem(s1), in_vmem(s2), in_vmem(fx), in_vmem(sya), in_vmem(syb), in_vmem(block), rya, ryb, rxa, rxb)
    p, im, sums = pl.pallas_call(
        fine_kernel,
        in_specs=[VM] * 18,
        out_specs=[VM] * 3,
        out_shape=[resident(4, (X + 2) * Y, LANES), resident(X * Y, Z), f32(LANES, 8)],
        scratch_shapes=[vm((2, X, Z), F32)],
        compiler_params=pltpu.CompilerParams(vmem_limit_bytes=8 * 2**20),
        name="solve_fine",
    )(in_vmem(r_v), in_vmem(d_v), in_vmem(s0), in_vmem(rep), in_vmem(faces), in_vmem(left),
      in_vmem(part), in_vmem(fx), in_vmem(sya), in_vmem(syb), in_vmem(sza), in_vmem(szb), rya, ryb, rza, rzb, rxa, rxb)

    every = lax.all_to_all(sums, ("gx", "gy"), 0, 0, tiled=True)
    blocks = pl.BlockSpec((OUT * Y, Z), lambda i: (i, 0))
    update, residual = pl.pallas_call(
        final_kernel,
        grid=(X // OUT,),
        in_specs=[VM] * 5,
        out_specs=[blocks, blocks],
        out_shape=[f32(X * Y, Z), f32(X * Y, Z)],
        compiler_params=pltpu.CompilerParams(vmem_limit_bytes=10 * 2**20),
        name="scale_outputs",
    )(every, in_vmem(r_v), in_vmem(d_v), in_vmem(p), in_vmem(im))
    return update.reshape(X, Y, Z), residual.reshape(X, Y, Z)


def solution(mesh):
    return jax.shard_map(
        body,
        mesh=mesh,
        in_specs=(P("gx", "gy", None), P("gx", "gy", None)),
        out_specs=(P("gx", "gy", None), P("gx", "gy", None)),
        check_vma=False,
    )
```

```python
import jax
import jax.numpy as jnp
from jax import lax
from jax.experimental import pallas as pl
from jax.experimental.pallas import tpu as pltpu
from jax.sharding import PartitionSpec as P


F32 = jnp.float32
BF16 = jnp.bfloat16

X, Y, Z = 64, 32, 512
DEVS_X, DEVS_Y = 8, 16
WHOLE = 512
LANES = 128
COST = 20_000_000
CHUNK = 16
OUT = 16

XF, XM, XL, XB, XC, XROWS = 0, 384, 480, 504, 664, 680
YF, YM, YL, YB, YROWS = 0, 256, 448, 496, 528
ZROWS = 512
SCALE = (1.0, 0.25, 0.0625)


def iota(shape, axis):
    return lax.broadcasted_iota(jnp.int32, shape, axis)


def halving(depth, cols, offset=0):
    coarse = lax.shift_right_logical(iota((depth, cols), 0), 1) + offset
    return jnp.where(coarse == iota((depth, cols), 1), 0.125, 0.0).astype(BF16)


def doubling(depth, cols):
    coarse = lax.shift_right_logical(iota((depth, cols), 1), 1)
    return jnp.where(coarse == iota((depth, cols), 0), 1.0, 0.0).astype(BF16)


def times(value, table):
    high = value.astype(BF16)
    low = (value - high.astype(F32)).astype(BF16)
    return jnp.dot(high, table, preferred_element_type=F32) + jnp.dot(low, table, preferred_element_type=F32)


def in_plane(c, top, bottom):
    rows, lanes = c.shape
    row, lane = iota(c.shape, 0), iota(c.shape, 1)
    up = jnp.where(row == 0, top, pltpu.roll(c, 1, 0))
    down = jnp.where(row == rows - 1, bottom, pltpu.roll(c, rows - 1, 0))
    left = jnp.where(lane == 0, 0.0, pltpu.roll(c, 1, 1))
    right = jnp.where(lane == lanes - 1, 0.0, pltpu.roll(c, lanes - 1, 1))
    return (up + down) + (left + right)


def cols(k):
    return slice(LANES * k, LANES * (k + 1))


def take(ref, rows):
    return jnp.concatenate([ref[k, rows, :] for k in range(ref.shape[0])], axis=1)


def put(ref, rows, value):
    for k in range(ref.shape[0]):
        ref[k, rows, :] = value[:, cols(k)]


def fold(v):
    v = (v[0:8] + v[8:16]) + (v[16:24] + v[24:32])
    return (v[:, cols(0)] + v[:, cols(1)]) + (v[:, cols(2)] + v[:, cols(3)])


def send(up, down, rows, low, high):
    up[rows, :] = high
    down[rows, :] = low


def beside(value, hi, axis, distance=1):
    index = lax.axis_index(axis)
    outside = index + distance >= lax.axis_size(axis) if hi else index < distance
    return jnp.where(outside, 0.0, value)


def restrict_kernel(r_hbm, d_hbm, r_v, d_v, g_s, i_s, fx, sya, syb, sza, szb, core, rm, gm, im, s2, part,
                    cm, rl, cl, gl, il, sems):
    def copies(c):
        rows = pl.ds(c * CHUNK * Y, CHUNK * Y)
        for n, (src, dst) in enumerate(((r_hbm, r_v), (d_hbm, d_v))):
            for k in range(4):
                yield pltpu.make_async_copy(src.at[rows, pl.ds(LANES * k, LANES)], dst.at[k, rows], sems.at[n, c, k])

    for c in range(X // CHUNK):
        for one in copies(c):
            one.start()

    for k in range(4):
        g_s[k, pl.ds(0, Y), :] = jnp.zeros((Y, LANES), F32)
        g_s[k, pl.ds((X + 1) * Y, Y), :] = jnp.zeros((Y, LANES), F32)
    for k in range(2):
        gm[k, pl.ds(0, 16), :] = jnp.zeros((16, LANES), F32)
        gm[k, pl.ds(33 * 16, 16), :] = jnp.zeros((16, LANES), F32)
    half = halving(512, 256)

    def load(c, carry):
        for one in copies(c):
            one.wait()
        base = c * CHUNK * Y

        def plane(i, carry):
            rows = pl.ds(base + i * Y, Y)
            dd, rr = take(d_v, rows), take(r_v, rows)
            inv = 0.8 / (6.0 + dd)
            put(i_s, rows, inv)
            put(g_s, pl.ds(base + (i + 1) * Y, Y), inv * rr)
            return carry[0] + fold(rr), carry[1] + fold(dd)

        carry = lax.fori_loop(0, CHUNK, plane, carry, unroll=4)
        n = CHUNK * Y // 2
        for src, dst in ((r_v, rm), (d_v, cm)):
            pairs = jnp.concatenate(
                [src[k, pl.ds(base, n, 2), :] + src[k, pl.ds(base + 1, n, 2), :] for k in range(4)], axis=1)
            pairs = pairs.reshape(CHUNK // 2, 2, 16, Z)
            pairs = (pairs[:, 0] + pairs[:, 1]).reshape(CHUNK // 2 * 16, Z)
            put(dst, pl.ds(c * (CHUNK // 2 * 16), CHUNK // 2 * 16), times(pairs, half))
        return carry

    start = jnp.zeros((8, LANES), F32)
    part[pl.ds(0, 8), :], part[pl.ds(8, 8), :] = lax.fori_loop(0, X // CHUNK, load, (start, start))

    half = halving(256, 128)
    for src, dst in ((rm, rl), (cm, cl)):
        pairs = jnp.concatenate([src[k, pl.ds(0, 256, 2), :] + src[k, pl.ds(1, 256, 2), :] for k in range(2)], axis=1)
        pairs = pairs.reshape(16, 2, 8, 256)
        pairs = (pairs[:, 0] + pairs[:, 1]).reshape(128, 256)
        dst[...] = times(pairs, half)
    packed = 0.0
    for src, offset in ((rl, 0), (cl, 64)):
        quad = [sum(src[pl.ds(8 * f + 2 * j + e, 8, 16), :] for e in range(2) for f in range(2)) for j in range(4)]
        packed = packed + times(jnp.concatenate(quad, axis=0), halving(128, 128, offset))
    core[...] = packed
    sya[pl.ds(YB, 32), :] = packed
    syb[pl.ds(YB, 32), :] = packed

    inv = 0.8 / (0.09375 * 4.0 + cl[...])
    il[...] = inv
    gl[...] = inv * rl[...]
    for i in range(16):
        rows = pl.ds(8 * i, 8)
        c = gl[rows, :]
        total = in_plane(c, 0.0, 0.0)
        if i > 0:
            total = total + gl[pl.ds(8 * i - 8, 8), :]
        if i < 15:
            total = total + gl[pl.ds(8 * i + 8, 8), :]
        s2[rows, :] = il[rows, :] * (1.2 * rl[rows, :] + 0.0625 * total)

    def guess(i, carry):
        rows = pl.ds(64 * i, 64)
        inv = 0.8 / (1.5 + take(cm, rows))
        put(im, rows, inv)
        put(gm, pl.ds(64 * i + 16, 64), inv * take(rm, rows))
        return carry

    lax.fori_loop(0, 8, guess, 0)

    def layer(ref, rows, pad):
        return take(ref, pl.ds(rows * pad, rows))

    for hi in range(2):
        for base, g, inv, res, n, last, level in ((XF, g_s, i_s, r_v, Y, X - 1, 0), (XM, gm, im, rm, 16, 31, 1)):
            i = last * hi
            c, v = layer(g, n, i + 1), layer(inv, n, i)
            total = in_plane(c, 0.0, 0.0) + layer(g, n, i + (0 if hi else 2))
            lanes = g.shape[0]
            for a, value in enumerate((c, v, v * (1.2 * layer(res, n, i) + SCALE[level] * total))):
                for k in range(lanes):
                    fx[hi, pl.ds(base + (lanes * a + k) * n, n), :] = value[:, cols(k)]
        for a, ref in enumerate((gl, il, s2)):
            fx[hi, pl.ds(XL + a * 8, 8), :] = ref[pl.ds(hi * 15 * 8, 8), :]

    for a, (shift, pad) in enumerate(((0, 1), (0, 0), (1, 1))):
        for base, ref, n, width in ((YF, (g_s, i_s, g_s)[a], X, Y), (YM, (gm, im, gm)[a], 32, 16)):
            lanes = ref.shape[0]
            for k in range(lanes):
                late = lanes == 4 and a > 0
                start = (4 * (a - 1) + k) * n if late else base + (lanes * a + k) * n
                send(sza if late else sya, szb if late else syb, pl.ds(start, n),
                     ref[k, pl.ds(pad * width + shift, n, width), :],
                     ref[k, pl.ds(pad * width + width - 1 - shift, n, width), :])
        ref = (gl, il, gl)[a]
        send(sya, syb, pl.ds(YL + a * 16, 16), ref[pl.ds(shift, 16, 8), :], ref[pl.ds(7 - shift, 16, 8), :])


def smooth_kernel(r_v, g_s, i_s, rm, gm, im, sza, szb, rya, ryb, s0, s1):
    def middle(i, carry):
        rows = pl.ds(16 * i, 16)
        c = take(gm, pl.ds(16 * i + 16, 16))
        total = in_plane(c, 0.0, 0.0) + (take(gm, rows) + take(gm, pl.ds(16 * i + 32, 16)))
        put(s1, rows, take(im, rows) * (1.2 * take(rm, rows) + 0.25 * total))
        return carry

    lax.fori_loop(0, 32, middle, 0, unroll=16)

    def fine(i, carry):
        rows = pl.ds(Y * i, Y)
        c = take(g_s, pl.ds(Y * i + Y, Y))
        total = in_plane(c, 0.0, 0.0) + (take(g_s, rows) + take(g_s, pl.ds(Y * i + 2 * Y, Y)))
        put(s0, rows, take(i_s, rows) * (1.2 * take(r_v, rows) + total))
        return carry

    lax.fori_loop(0, X, fine, 0, unroll=8)
    halo = Halo(sz=(sza, szb), ry=(rya, ryb))
    for hi in range(2):
        for k in range(4):
            rows = pl.ds(hi * (Y - 1), X, Y)
            s0[k, rows, :] = s0[k, rows, :] + halo.get("sz", hi, k * X, X) * halo.get("ry", hi, YF + k * X, X)


class Halo:
    def __init__(self, **pairs):
        self.pairs = pairs

    def get(self, name, hi, start, n):
        value = self.pairs[name][1 - hi][pl.ds(start, n), :]
        if name[0] == "s":
            return value
        return beside(value, hi, "gx" if name == "rx" else "gy")

    def layer(self, name, hi, start, n, lanes):
        return jnp.concatenate([self.get(name, hi, start + k * n, n) for k in range(lanes)], axis=1)

    def smoothed(self, along_y, hi, level, fx):
        lanes, n = 4 >> level, (X if along_y else Y) >> level
        if along_y:
            base = (YF, YM, YL)[level]
            if level == 0:
                g = self.layer("ry", hi, base, n, lanes)
                inv, beyond = [self.layer("rz", hi, a * lanes * n, n, lanes) for a in range(2)]
            else:
                g, inv, beyond = [self.layer("ry", hi, base + a * lanes * n, n, lanes) for a in range(3)]
            first, last = [self.layer("rx", xhi, XC + 7 * hi + (0, 4, 6)[level], 1, lanes) for xhi in range(2)]
            around = in_plane(g, first, last) + (beyond + self.layer("sy", hi, base, n, lanes))
            return 1.2 * g + SCALE[level] * inv * around, inv
        base = (XF, XM, XL)[level]
        inv, partly = [self.layer("rx", hi, base + a * lanes * n, n, lanes) for a in (1, 2)]
        own = jnp.concatenate([fx[hi, pl.ds(base + k * n, n), :] for k in range(lanes)], axis=1)
        return partly + SCALE[level] * inv * own, inv


def pack_kernel(fx, core, rya, ryb, r2a, r2b, block, outa, outb):
    halo = Halo(ry=(rya, ryb))
    block[pl.ds(0, 32), :] = beside(r2b[...], 0, "gy", 2)
    block[pl.ds(32, 32), :] = halo.get("ry", 0, YB, 32)
    block[pl.ds(64, 32), :] = core[...]
    block[pl.ds(96, 32), :] = halo.get("ry", 1, YB, 32)
    block[pl.ds(128, 32), :] = beside(r2a[...], 1, "gy", 2)
    for out in (outa, outb):
        out[pl.ds(XB, 160), :] = block[...]
    sides = []
    for hi in range(2):
        rows, corner = [[], []], []
        for level, (base, ybase) in enumerate(((XF, YF), (XM, YM), (XL, YL))):
            lanes, n, long = 4 >> level, Y >> level, X >> level
            rows.append(fx[hi, pl.ds(base, 2 * lanes * n), :])
            edges = [[halo.get("ry", yhi, ybase + k * long + hi * (long - 1), 1) for yhi in range(2)] for k in range(lanes)]
            for k in range(lanes):
                inv = fx[hi, pl.ds(base + (lanes + k) * n, n), :]
                partly = fx[hi, pl.ds(base + (2 * lanes + k) * n, n), :]
                rows.append(partly + SCALE[level] * inv * ends(n, *edges[k]))
                for yhi in range(2):
                    rows[yhi].append(edges[k][yhi])
        corner = rows[0] + rows[1] + [jnp.zeros((2, LANES), F32)]
        sides.append((jnp.concatenate(rows[2:], axis=0), jnp.concatenate(corner, axis=0)))
    send(outa, outb, pl.ds(0, XB), sides[0][0], sides[1][0])
    send(outa, outb, pl.ds(XC, 16), sides[0][1], sides[1][1])


def ends(rows, first, last):
    row = iota((rows, LANES), 0)
    return jnp.where(row == 0, first, jnp.where(row == rows - 1, last, 0.0))


FACES = ((False, 0), (False, 1), (True, 0), (True, 1))
FACE_ROWS = (0, Y, 2 * Y, 2 * Y + X)


def coarse_kernel(s1, s2, fx, sya, syb, block, rya, ryb, rxa, rxb,
                  rep_m, fm, left_out,
                  bs, ga, gb, sz, low_s, rep_l, mid_s, fl):
    halo = Halo(sy=(sya, syb), rx=(rxa, rxb), ry=(rya, ryb))

    for n, value in enumerate((halo.get("rx", 0, XB, 160), block[...], halo.get("rx", 1, XB, 160))):
        bs[:, pl.ds(8 * n, 8), :] = value.reshape(20, 8, LANES)
    shape = (20, 24, LANES)
    live = iota(shape, 2) < 64
    both = bs[...]
    res = jnp.where(live, both, 0.0)
    coef = jnp.where(live, pltpu.roll(both, 64, 2), 0.0)
    inv = jnp.where(coef > 0.0, 0.8 / (0.09375 + coef), 0.0)
    zero = jnp.zeros((24, LANES), F32)
    for ref in (ga, gb):
        ref[0] = zero
        ref[21] = zero

    def around(ref):
        c = ref[pl.ds(1, 20)]
        total = ref[pl.ds(0, 20)] + ref[pl.ds(2, 20)]
        total = total + (pltpu.roll(c, 1, 1) + pltpu.roll(c, 23, 1))
        return c, total + (pltpu.roll(c, 1, 2) + pltpu.roll(c, LANES - 1, 2))

    ga[pl.ds(1, 20)] = inv * res
    bs[...] = inv
    now, new = ga, gb
    for _ in range(7):
        c, total = around(now)
        new[pl.ds(1, 20)] = c + bs[...] * (res - ((0.09375 + coef) * c - 0.015625 * total))
        now, new = new, now
    c, total = around(now)
    left = res - ((0.09375 + coef) * c - 0.015625 * total)
    leftover = jnp.sum(jnp.where(live[8:12, 8:16], left[8:12, 8:16], 0.0))
    sz[...] = times(now[pl.ds(8, 6)].reshape(144, LANES), doubling(LANES, LANES))

    left_out[...] = jnp.full((8, LANES), leftover, F32)

    for j in range(4):
        for e in range(2):
            for f in range(2):
                low_s[pl.ds(8 * f + 2 * j + e, 8, 16), :] = sz[pl.ds(24 * (j + 1) + 8, 8), :]
    low_s[...] = low_s[...] + s2[...]
    for hi in range(2):
        rows = pl.ds(hi * 120, 8)
        low_s[rows, :] = low_s[rows, :] + 0.0625 * fx[hi, pl.ds(XL + 8, 8), :] * halo.get("rx", hi, XL, 8)
    for hi in range(2):
        rows = pl.ds(hi * 7, 16, 8)
        low_s[rows, :] = low_s[rows, :] + 0.0625 * halo.get("sy", hi, YL + 16, 16) * halo.get("ry", hi, YL, 16)

    rep_l[pl.ds(0, 128, 2), :] = low_s[...]
    rep_l[pl.ds(1, 128, 2), :] = low_s[...]
    wide = times(rep_l[...], doubling(128, 256)).reshape(16, 1, 16, 256)
    wide = jnp.broadcast_to(wide, (16, 2, 16, 256)).reshape(512, 256)
    for k in range(2):
        mid_s[k] = wide[:, cols(k)] + s1[k]
    for hi in range(2):
        for k in range(2):
            rows = pl.ds(hi * 496, 16)
            mid_s[k, rows, :] = mid_s[k, rows, :] + (
                0.25 * fx[hi, pl.ds(XM + 32 + 16 * k, 16), :] * halo.get("rx", hi, XM + 16 * k, 16))
    for hi in range(2):
        for k in range(2):
            rows = pl.ds(hi * 15, 32, 16)
            mid_s[k, rows, :] = mid_s[k, rows, :] + (
                0.25 * halo.get("sy", hi, YM + 64 + 32 * k, 32) * halo.get("ry", hi, YM + 32 * k, 32))

    for k in range(2):
        rep_m[k, pl.ds(0, 512, 2), :] = mid_s[k]
        rep_m[k, pl.ds(1, 512, 2), :] = mid_s[k]
    for (along_y, hi), base in zip(FACES, FACE_ROWS):
        n = X if along_y else Y
        n2, n1 = n // 4, n // 2
        if along_y:
            top = sz[pl.ds(120 * hi + 8, 8), :]
        else:
            top = sz[pl.ds(24 + (16 if hi else 7), 4, 24), :]
        fl[pl.ds(0, n2 // 2, 2), :] = top
        fl[pl.ds(1, n2 // 2, 2), :] = top
        low = halo.smoothed(along_y, hi, 2, fx)[0] + fl[pl.ds(0, n2), :]
        fl[pl.ds(0, n2, 2), :] = low
        fl[pl.ds(1, n2, 2), :] = low
        wide = times(fl[pl.ds(0, n1), :], doubling(128, 256))
        middle = halo.smoothed(along_y, hi, 1, fx)[0] + wide
        for k in range(2):
            mid = middle[:, cols(k)]
            fm[k, pl.ds(base, n1, 2), :] = mid
            fm[k, pl.ds(base + 1, n1, 2), :] = mid


def fine_kernel(r_v, d_v, s0, rep_m, fm, left_in, part, fx, sya, syb, rya, ryb, rza, rzb, rxa, rxb,
                p, im, sums, hy):
    halo = Halo(sy=(sya, syb), rx=(rxa, rxb), ry=(rya, ryb), rz=(rza, rzb))
    twice = doubling(256, Z)

    def spread(i, carry):
        wide = times(take(rep_m, pl.ds(128 * i, 128)), twice).reshape(4, 1, Y, Z)
        wide = jnp.broadcast_to(wide, (4, 2, Y, Z)).reshape(8 * Y, Z)
        for k in range(4):
            p[k, pl.ds(8 * Y * i + Y, 8 * Y), :] = wide[:, cols(k)] + s0[k, pl.ds(8 * Y * i, 8 * Y), :]
        return carry

    lax.fori_loop(0, 8, spread, 0, unroll=2)
    for hi in range(2):
        for k in range(4):
            rows = pl.ds(Y + hi * (X - 1) * Y, Y)
            p[k, rows, :] = p[k, rows, :] + fx[hi, pl.ds(XF + (4 + k) * Y, Y), :] * halo.get("rx", hi, XF + k * Y, Y)
    outer = times(take(fm, pl.ds(0, 2 * (X + Y))), twice)
    for (along_y, hi), base in zip(FACES, FACE_ROWS):
        n = X if along_y else Y
        value, inv = halo.smoothed(along_y, hi, 0, fx)
        value = jnp.where(inv > 0.0, value + outer[base:base + n], 0.0)
        if along_y:
            hy[hi] = value
        else:
            put(p, pl.ds(hi * (X + 1) * Y, Y), value)

    def image(i, carry):
        rows = pl.ds(Y * i, Y)
        c = take(p, pl.ds(Y * i + Y, Y))
        around = in_plane(c, hy[0, pl.ds(i, 1), :], hy[1, pl.ds(i, 1), :])
        around = around + (take(p, rows) + take(p, pl.ds(Y * i + 2 * Y, Y)))
        dd, rr = take(d_v, rows), take(r_v, rows)
        out = (6.0 + dd) * c - around
        im[rows, :] = out
        return tuple(t + fold(v) for t, v in zip(carry, (rr * c, c * out, out)))

    start = jnp.zeros((8, LANES), F32)
    totals = lax.fori_loop(0, X, image, (start,) * 3, unroll=8)
    rz, zq, image_sum = [jnp.sum(t) for t in totals]
    totals = [rz, zq, jnp.sum(part[pl.ds(0, 8), :]), image_sum, jnp.sum(part[pl.ds(8, 8), :]), left_in[0:1, 0:1]]
    lane = iota((LANES, 8), 1)
    packed = jnp.zeros((LANES, 8), F32)
    for n, t in enumerate(totals):
        packed = jnp.where(lane == n, t, packed)
    sums[...] = packed


def final_kernel(every, r_v, d_v, p, im, update, residual):
    step = pl.program_id(0)
    gx, gy = lax.axis_index("gx"), lax.axis_index("gy")
    total = jnp.sum(every[...], axis=0, keepdims=True)
    lane8 = iota((1, 8), 1)
    rz, zq, res_sum, image_sum, coef_sum, left = [jnp.sum(jnp.where(lane8 == n, total, 0.0), axis=1, keepdims=True) for n in range(6)]
    shift = left / (coef_sum / 512.0 + 6.0 * 64.0 * 64.0 / 64.0)
    ones_sum = coef_sum + 6.0 * WHOLE * WHOLE
    alpha = (rz + shift * res_sum) / (zq + shift * (2.0 * image_sum + shift * ones_sum))
    scaled = alpha * shift
    row, lane = iota((Y, Z), 0), iota((Y, Z), 1)
    walls = jnp.where(lane == 0, 1.0, 0.0) + jnp.where(lane == Z - 1, 1.0, 0.0)
    walls = walls + jnp.where((row == 0) & (gy == 0), 1.0, 0.0)
    walls = walls + jnp.where((row == Y - 1) & (gy == DEVS_Y - 1), 1.0, 0.0)

    def plane(i, carry):
        x = step * OUT + i
        end = ((x == 0) & (gx == 0)) | ((x == X - 1) & (gx == DEVS_X - 1))
        rows = pl.ds(x * Y, Y)
        outside = walls + jnp.where(end, 1.0, 0.0)
        here = pl.ds(i * Y, Y)
        update[here, :] = alpha * take(p, pl.ds(x * Y + Y, Y)) + scaled
        residual[here, :] = take(r_v, rows) - alpha * im[rows, :] - scaled * (take(d_v, rows) + outside)
        return carry

    lax.fori_loop(0, OUT, plane, 0, unroll=8)


def f32(*shape):
    return jax.ShapeDtypeStruct(shape, F32)


def resident(*shape):
    return pltpu.VMEM(shape, F32)


def in_vmem(value):
    return pltpu.with_memory_space_constraint(value, pltpu.VMEM)


VM = pl.BlockSpec(memory_space=pltpu.VMEM)


def shift(value, axis, distance):
    count = lax.axis_size(axis)
    return lax.ppermute(value, axis, [(i, (i + distance) % count) for i in range(count)])


def body(right_side, diagonal):
    r = right_side.reshape(X * Y, Z)
    d = diagonal.reshape(X * Y, Z)
    vm = pltpu.VMEM
    hbm = pl.BlockSpec(memory_space=pl.ANY)
    r_v, d_v, g, inv, fx, sya, syb, sza, szb, core, rm, gm, im1, s2, part = pl.pallas_call(
        restrict_kernel,
        in_specs=[hbm, hbm],
        out_specs=[VM] * 15,
        out_shape=[resident(4, X * Y, LANES)] * 2 + [resident(4, (X + 2) * Y, LANES), resident(4, X * Y, LANES)]
        + [resident(2, XB, LANES)] + [resident(YROWS, LANES)] * 2 + [resident(ZROWS, LANES)] * 2 + [resident(32, LANES), resident(2, 512, LANES)]
        + [resident(2, 544, LANES), resident(2, 512, LANES), resident(128, 128), resident(16, LANES)],
        scratch_shapes=[vm((2, 512, LANES), F32)] + [vm((128, 128), F32)] * 4
        + [pltpu.SemaphoreType.DMA((2, X // CHUNK, 4))],
        compiler_params=pltpu.CompilerParams(vmem_limit_bytes=12 * 2**20),
        name="restrict_all",
    )(pltpu.with_memory_space_constraint(r, pltpu.HBM), pltpu.with_memory_space_constraint(d, pltpu.HBM))

    rya = shift(syb, "gy", -1)
    ryb = shift(sya, "gy", 1)
    r2a = shift(core, "gy", -2)
    r2b = shift(core, "gy", 2)
    s0, s1 = pl.pallas_call(
        smooth_kernel,
        in_specs=[VM] * 10,
        out_specs=[VM] * 2,
        out_shape=[resident(4, X * Y, LANES), resident(2, 512, LANES)],
        compiler_params=pltpu.CompilerParams(vmem_limit_bytes=4 * 2**20),
        cost_estimate=pl.CostEstimate(flops=COST, transcendentals=0, bytes_accessed=0),
        name="smooth_own",
    )(in_vmem(r_v), in_vmem(g), in_vmem(inv), in_vmem(rm), in_vmem(gm), in_vmem(im1), in_vmem(sza), in_vmem(szb), rya, ryb)
    block, outa, outb = pl.pallas_call(
        pack_kernel,
        in_specs=[VM] * 6,
        out_specs=[VM] * 3,
        out_shape=[resident(160, LANES)] + [resident(XROWS, LANES)] * 2,
        compiler_params=pltpu.CompilerParams(vmem_limit_bytes=2 * 2**20),
        name="pack_faces",
    )(in_vmem(fx), in_vmem(core), rya, ryb, r2a, r2b)
    rxa = shift(outb, "gx", -1)
    rxb = shift(outa, "gx", 1)
    rza = shift(szb, "gy", -1)
    rzb = shift(sza, "gy", 1)

    rep, faces, left = pl.pallas_call(
        coarse_kernel,
        in_specs=[VM] * 10,
        out_specs=[VM] * 3,
        out_shape=[resident(2, 1024, LANES), resident(2, 2 * (X + Y), LANES), resident(8, LANES)],
        scratch_shapes=[vm((20, 24, LANES), F32), vm((22, 24, LANES), F32), vm((22, 24, LANES), F32), vm((144, LANES), F32),
                        vm((128, 128), F32), vm((256, 128), F32), vm((2, 512, LANES), F32), vm((32, LANES), F32)],
        compiler_params=pltpu.CompilerParams(vmem_limit_bytes=8 * 2**20),
        cost_estimate=pl.CostEstimate(flops=COST, transcendentals=0, bytes_accessed=0),
        name="solve_coarse",
    )(in_vmem(s1), in_vmem(s2), in_vmem(fx), in_vmem(sya), in_vmem(syb), in_vmem(block), rya, ryb, rxa, rxb)
    p, im, sums = pl.pallas_call(
        fine_kernel,
        in_specs=[VM] * 16,
        out_specs=[VM] * 3,
        out_shape=[resident(4, (X + 2) * Y, LANES), resident(X * Y, Z), f32(LANES, 8)],
        scratch_shapes=[vm((2, X, Z), F32)],
        compiler_params=pltpu.CompilerParams(vmem_limit_bytes=8 * 2**20),
        name="solve_fine",
    )(in_vmem(r_v), in_vmem(d_v), in_vmem(s0), in_vmem(rep), in_vmem(faces), in_vmem(left),
      in_vmem(part), in_vmem(fx), in_vmem(sya), in_vmem(syb), rya, ryb, rza, rzb, rxa, rxb)

    every = lax.all_to_all(sums, ("gx", "gy"), 0, 0, tiled=True)
    blocks = pl.BlockSpec((OUT * Y, Z), lambda i: (i, 0))
    update, residual = pl.pallas_call(
        final_kernel,
        grid=(X // OUT,),
        in_specs=[VM] * 5,
        out_specs=[blocks, blocks],
        out_shape=[f32(X * Y, Z), f32(X * Y, Z)],
        compiler_params=pltpu.CompilerParams(vmem_limit_bytes=10 * 2**20),
        name="scale_outputs",
    )(every, in_vmem(r_v), in_vmem(d_v), in_vmem(p), in_vmem(im))
    return update.reshape(X, Y, Z), residual.reshape(X, Y, Z)


def solution(mesh):
    return jax.shard_map(
        body,
        mesh=mesh,
        in_specs=(P("gx", "gy", None), P("gx", "gy", None)),
        out_specs=(P("gx", "gy", None), P("gx", "gy", None)),
        check_vma=False,
    )
```
